32 devices in a mesh: inner: 4 (over x, core), outer: 8 (over z, y).
Axes of the slice: x: 2, y: 2, z: 4, core: 2. Of those that a mesh axis runs over, the one named last changes fastest.
Arguments:
- queries: bfloat16 [8192, 512], P(('inner', 'outer')), may hold values from -12 to 12
- keys: bfloat16 [8192, 128], P(('inner', 'outer')), may hold values from -12 to 12
- values: bfloat16 [8192, 128], P(('inner', 'outer')), may hold values from -6 to 6
- out_grad: bfloat16 [8192, 512], P(('inner', 'outer')), may hold values from -6 to 6
- block_place: int32 [64], replicated, may hold values from 0 to 63, each once
Outputs:
- query_grad: bfloat16 [8192, 512], P(('inner', 'outer'))
- key_grad: bfloat16 [8192, 128], P(('inner', 'outer'))
- value_grad: bfloat16 [8192, 128], P(('inner', 'outer'))
The draws below stay inside these ranges and needn't reach their ends.
Inputs may be any that keep to these rules, and one draw needn't show every extreme that they name: `block_place`: every block place appears exactly once.
All inputs are finite; a program needn't handle non-finite values.
Results may differ from the reference program's by a relative error of at most 0.017.
Values may be sent and summed in bfloat16 or wider, within the bound.
No kernel may reach another device: no remote copies, remote signals or barrier semaphores. Data moves between devices by JAX's collectives and lax.ppermute only.
A program may use at most 128 MiB of HBM per device.

```python
import math
import jax
import jax.numpy as jnp
from jax import lax

HD = 128
HEADS = 4
TOK_DEV = 256
STEPS = 4
SEQ = 8192
BLOCKS = 64
N_INNER = 4
N_OUTER = 8


def shared_keys(key):
    normals = jax.random.normal(jax.random.fold_in(key, 11), (SEQ, HD), jnp.float32)
    normals = jnp.clip(normals, -6.0, 6.0)
    return normals


def draw_keys(key, part):
    return shared_keys(key).astype(jnp.bfloat16)


def draw_queries(key, part):
    normals = jnp.clip(jax.random.normal(jax.random.fold_in(key, 12), (SEQ, HEADS, HD), jnp.float32), -6.0, 6.0)
    return normals.reshape(SEQ, HEADS * HD).astype(jnp.bfloat16)


def shard_levels(key, dims, cuts, least, largest):
    factor_of, own = 1.0, jax.random.fold_in(key, 6)
    for axis_at, blocks in cuts:
        heights = jnp.exp(jax.random.uniform(jax.random.fold_in(own, axis_at), (blocks,), jnp.float32, least / len(cuts), largest / len(cuts)))
        factor_of = factor_of * jnp.repeat(heights, dims[axis_at] // blocks).reshape([-1 if axis == axis_at else 1 for axis in range(len(dims))])
    return factor_of


def centred(rng, extent, spread, most, cuts=(), held_as=jnp.bfloat16):
    drawn = jax.random.normal(rng, extent, jnp.float32) * spread
    if len(cuts) > 0:
        drawn = shard_levels(rng, extent, cuts, -0.22, 0.18) * drawn
    return jnp.clip(drawn, min=-most, max=most).astype(held_as)


def setup_inputs(seed: int = 0) -> dict:
    key_list = jax.random.split(jax.random.key(seed), 6)
    queries = draw_queries(jax.random.fold_in(key_list[5], 71), 0)
    keys = draw_keys(jax.random.fold_in(key_list[5], 71), 0)
    values = centred(key_list[2], (SEQ, HD), 1.0, 6.0, ((0, 32),))
    out_grad = centred(key_list[3], (SEQ, HEADS * HD), 1.0, 6.0, ((0, 32),))
    block_place = jax.random.permutation(key_list[4], BLOCKS).astype(jnp.int32)
    return dict(queries=queries, keys=keys, values=values, out_grad=out_grad, block_place=block_place)


def reference(queries, keys, values, out_grad, block_place):
    all_rows = keys.shape[0]
    head_size = keys.shape[1]
    row_count = TOK_DEV
    block_len = row_count // 2
    group_rows = N_INNER * row_count
    score_scale = 1.0 / math.sqrt(head_size)
    offsets = jnp.arange(block_len, dtype=jnp.int32)
    place = (block_place.astype(jnp.int32)[:, None] * block_len + offsets[None, :]).reshape(all_rows)
    place_grid = place.reshape(N_INNER, N_OUTER, row_count)
    key_grid = keys.astype(jnp.float32).reshape(N_INNER, N_OUTER, row_count, head_size)
    value_grid = values.astype(jnp.float32).reshape(N_INNER, N_OUTER, row_count, head_size)
    query_grid = queries.astype(jnp.float32).reshape(N_INNER, N_OUTER, row_count, HEADS, head_size)
    grad_grid = out_grad.astype(jnp.float32).reshape(N_INNER, N_OUTER, row_count, HEADS, head_size)

    def window(grid, group):
        pieces = []
        for step in range(STEPS):
            source = ((group - step) % N_OUTER).astype(jnp.int32)
            pieces.append(lax.dynamic_index_in_dim(grid, source, 1, False))
        whole = jnp.stack(pieces, axis=0)
        return whole.reshape((STEPS * group_rows,) + grid.shape[3:])

    def one_device(state, device):
        key_acc, value_acc = state
        inner_i = (device // N_OUTER).astype(jnp.int32)
        group = (device % N_OUTER).astype(jnp.int32)
        query_f = lax.dynamic_index_in_dim(lax.dynamic_index_in_dim(query_grid, inner_i, 0, False), group, 0, False)
        grad_f = lax.dynamic_index_in_dim(lax.dynamic_index_in_dim(grad_grid, inner_i, 0, False), group, 0, False)
        query_place = lax.dynamic_index_in_dim(lax.dynamic_index_in_dim(place_grid, inner_i, 0, False), group, 0, False)
        keys_f = window(key_grid, group)
        values_f = window(value_grid, group)
        key_place = window(place_grid, group)
        scores = jnp.einsum('thd,kd->thk', query_f, keys_f) * score_scale
        allowed = key_place[None, None, :] <= query_place[:, None, None]
        scores = jnp.where(allowed, scores, -1e+30)
        row_max = lax.optimization_barrier(jnp.max(scores, axis=-1))
        log_total = row_max + jnp.log(lax.optimization_barrier(jnp.sum(jnp.where(allowed, jnp.exp(scores - row_max[..., None]), 0.0), axis=-1)))
        probs = jnp.where(allowed, jnp.exp(scores - log_total[..., None]), 0.0)
        probs_low = probs.astype(jnp.bfloat16)
        probs_low_f = probs_low.astype(jnp.float32)
        attended = jnp.einsum('thk,kd->thd', probs_low_f, values_f)
        row_dot = lax.optimization_barrier(jnp.sum(grad_f * attended, axis=-1))
        grad_probs = jnp.einsum('thd,kd->thk', grad_f, values_f)
        grad_scores = (probs * (grad_probs - row_dot[..., None])).astype(jnp.bfloat16)
        grad_scores_f = grad_scores.astype(jnp.float32)
        query_grad = (jnp.einsum('thk,kd->thd', grad_scores_f, keys_f) * score_scale).astype(jnp.bfloat16)
        key_part = (jnp.einsum('thk,thd->kd', grad_scores_f, query_f) * score_scale).reshape(STEPS, N_INNER, 1, row_count, head_size)
        value_part = jnp.einsum('thk,thd->kd', probs_low_f, grad_f).reshape(STEPS, N_INNER, 1, row_count, head_size)
        zero_index = jnp.zeros((), jnp.int32)
        for step in range(STEPS):
            source = ((group - step) % N_OUTER).astype(jnp.int32)
            corner = (zero_index, source, zero_index, zero_index)
            size = (N_INNER, 1, row_count, head_size)
            key_acc = lax.dynamic_update_slice(key_acc, lax.dynamic_slice(key_acc, corner, size) + key_part[step], corner)
            value_acc = lax.dynamic_update_slice(value_acc, lax.dynamic_slice(value_acc, corner, size) + value_part[step], corner)
        return ((key_acc, value_acc), query_grad.reshape(row_count, HEADS * head_size))
    zero_grid = jnp.zeros((N_INNER, N_OUTER, row_count, head_size), jnp.float32)
    devices = jnp.arange(N_INNER * N_OUTER, dtype=jnp.int32)
    (key_acc, value_acc), query_parts = lax.scan(one_device, (zero_grid, zero_grid), devices)
    query_grad = query_parts.reshape(all_rows, HEADS * head_size)
    return (query_grad, key_acc.reshape(all_rows, head_size).astype(jnp.bfloat16), value_acc.reshape(all_rows, head_size).astype(jnp.bfloat16))
```

```python
import functools
import math

import jax
import jax.numpy as jnp
from jax import lax
from jax.experimental import pallas as pl
from jax.experimental.pallas import tpu as pltpu
from jax.sharding import PartitionSpec as P

STEPS = 4
NEG = -1e30
LOG2E = math.log2(math.e)
NT = (((1,), (1,)), ((), ()))


def dot_nt(a, b):
    return lax.dot_general(a, b, NT, preferred_element_type=jnp.float32)


def from_behind(block, axis, distance):
    devices = range(lax.axis_size(axis))
    route = [((i - distance) % len(devices), i) for i in devices]
    return lax.ppermute(block, axis, route)


def swap(block, axis, bit):
    return lax.ppermute(block, axis, [(i, i ^ bit) for i in range(lax.axis_size(axis))])


def fill_bias(bias_ref):
    size = bias_ref.shape[1]
    key_off = lax.broadcasted_iota(jnp.int32, (size, size), 0)
    query_off = lax.broadcasted_iota(jnp.int32, (size, size), 1)
    bias_ref[0] = jnp.zeros((size, size), jnp.float32)
    bias_ref[1] = jnp.where(key_off <= query_off, 0.0, NEG).astype(jnp.float32)
    bias_ref[2] = jnp.full((size, size), NEG, jnp.float32)


def build_lists(sizes, place_ref, where_ref, list_ref, count_ref):
    outer_size, key_blocks = sizes
    inner, outer = where_ref[0], where_ref[1]
    key_place = []
    for block in range(key_blocks):
        step, core, half = block // 4, (block // 2) % 2, block % 2
        source = lax.rem(outer - step + outer_size, outer_size)
        holder = inner if core == 0 else where_ref[2]
        key_place.append(place_ref[(holder * outer_size + source) * 2 + half])
    for query in range(4):
        holder = inner if query < 2 else where_ref[3]
        query_place = place_ref[(holder * outer_size + outer) * 2 + query % 2]
        count = jnp.int32(0)
        for block in range(key_blocks):
            kind = jnp.where(key_place[block] == query_place, 1, 0)
            list_ref[query, count] = block * 4 + kind
            count = count + jnp.where(key_place[block] <= query_place, 1, 0)
        list_ref[query, count] = 2
        count_ref[query] = (count + 1) // 2


def load_rows(src_refs, dst_ref, heads, size):
    for which, src in enumerate(src_refs):
        for half in range(2):
            for head in range(heads):
                dst_ref[which * 2 + half, pl.ds(head * size, size), :] = src[
                    pl.ds(half * size, size), pl.ds(head * size, size)
                ]


def stats_kernel(
    sizes, scale, place_ref, where_ref, q0, q1, g0, g1, *rest
):
    heads, size, outer_size, key_blocks = sizes
    shards = key_blocks // 2
    kv_hbm = rest[:shards]
    out_ref, qs, gs, kv, bias, lists, counts, sems = rest[shards:]
    copies = [pltpu.make_async_copy(kv_hbm[i], kv.at[i], sems.at[i]) for i in range(shards)]
    for copy in copies:
        copy.start()
    build_lists((outer_size, key_blocks), place_ref, where_ref, lists, counts)
    fill_bias(bias)
    load_rows((q0, q1), qs, heads, size)
    load_rows((g0, g1), gs, heads, size)
    for copy in copies:
        copy.wait()
    width = 2 * size
    chunks = heads // 2
    factor = scale * LOG2E

    @pl.loop(0, 4)
    def _(query):
        def step(index, carry):
            e0, e1 = lists[query, 2 * index], lists[query, 2 * index + 1]
            j0, j1 = e0 // 4, e1 // 4
            r0 = kv[j0 // 2, pl.ds(pl.multiple_of((j0 % 2) * size, size), size), :]
            r1 = kv[j1 // 2, pl.ds(pl.multiple_of((j1 % 2) * size, size), size), :]
            rows = jnp.concatenate([r0, r1], axis=0)
            k2, v2 = rows[:, :size], rows[:, size:]
            b2 = jnp.concatenate([bias[e0 % 4], bias[e1 % 4]], axis=0)
            b2 = jnp.concatenate([b2, b2], axis=1)
            out = []
            for c in range(chunks):
                m, l, r = carry[c]
                qc = qs[query, pl.ds(c * width, width), :]
                gc = gs[query, pl.ds(c * width, width), :]
                t = dot_nt(k2, qc) * factor + b2
                dp = dot_nt(v2, gc)
                m_new = jnp.maximum(m, jnp.max(t, axis=0, keepdims=True))
                corr = jnp.exp2(m - m_new)
                p = jnp.exp2(t - m_new)
                l = l * corr + jnp.sum(p.reshape(-1, 8, width), axis=0)
                r = r * corr + jnp.sum((p * dp).reshape(-1, 8, width), axis=0)
                out.append((m_new, l, r))
            return tuple(out)

        start = tuple(
            (
                jnp.full((1, width), NEG, jnp.float32),
                jnp.zeros((8, width), jnp.float32),
                jnp.zeros((8, width), jnp.float32),
            )
            for _ in range(chunks)
        )
        done = lax.fori_loop(0, counts[query], step, start)
        for c in range(chunks):
            m, l, r = done[c]
            out_ref[query, 0:1, pl.ds(c * width, width)] = m
            out_ref[query, 1:2, pl.ds(c * width, width)] = jnp.sum(l, axis=0, keepdims=True)
            out_ref[query, 2:3, pl.ds(c * width, width)] = jnp.sum(r, axis=0, keepdims=True)
            out_ref[query, 3:8, pl.ds(c * width, width)] = jnp.zeros((5, width), jnp.float32)


def grads_kernel(
    sizes, scale, place_ref, where_ref, mine, other, q0, q1, g0, g1, *rest
):
    heads, size, outer_size, key_blocks = sizes
    shards = key_blocks // 2
    steps = shards // 2
    kv_hbm = rest[:shards]
    rest = rest[shards:]
    dq_own, dq_sent = rest[0], rest[1]
    own_out, sent_out = rest[2 : 2 + steps], rest[2 + steps : 2 + 2 * steps]
    qs, gs, kv, kt, dk, dv, dq, base, bias, lists, counts, sems = rest[2 + 2 * steps :]
    copies = [pltpu.make_async_copy(kv_hbm[i], kv.at[i], sems.at[i]) for i in range(shards)]
    for copy in copies:
        copy.start()
    build_lists((outer_size, key_blocks), place_ref, where_ref, lists, counts)
    fill_bias(bias)
    load_rows((q0, q1), qs, heads, size)
    load_rows((g0, g1), gs, heads, size)
    for query in range(4):
        a, b = mine[query], other[query ^ 2]
        m = jnp.maximum(a[0:1], b[0:1])
        ea, eb = jnp.exp2(a[0:1] - m), jnp.exp2(b[0:1] - m)
        total = a[1:2] * ea + b[1:2] * eb
        base[query, 0:1] = m + jnp.log2(total)
        base[query, 1:2] = (a[2:3] * ea + b[2:3] * eb) / total
    dk[...] = jnp.zeros_like(dk)
    dv[...] = jnp.zeros_like(dv)
    for i, copy in enumerate(copies):
        copy.wait()
        for half in range(2):
            kt[2 * i + half] = kv[i, pl.ds(half * size, size), pl.ds(0, size)].T
    width = 2 * size
    chunks = heads // 2
    factor = scale * LOG2E

    @pl.loop(0, 4)
    def _(query):
        dq[...] = jnp.zeros_like(dq)

        @pl.loop(0, counts[query])
        def _(index):
            e0, e1 = lists[query, 2 * index], lists[query, 2 * index + 1]
            j0, j1 = e0 // 4, e1 // 4
            r0 = kv[j0 // 2, pl.ds(pl.multiple_of((j0 % 2) * size, size), size), :]
            r1 = kv[j1 // 2, pl.ds(pl.multiple_of((j1 % 2) * size, size), size), :]
            rows = jnp.concatenate([r0, r1], axis=0)
            k2, v2 = rows[:, :size], rows[:, size:]
            kt2 = jnp.concatenate([kt[j0], kt[j1]], axis=1)
            b2 = jnp.concatenate([bias[e0 % 4], bias[e1 % 4]], axis=0)
            b2 = jnp.concatenate([b2, b2], axis=1)
            dk_sum, dv_sum = None, None
            for c in range(chunks):
                at = pl.ds(c * width, width)
                qc, gc = qs[query, at, :], gs[query, at, :]
                t = dot_nt(k2, qc) * factor + b2
                dp = dot_nt(v2, gc)
                p = jnp.exp2(t - base[query, 0:1, at])
                ds = (p * (dp - base[query, 1:2, at])).astype(jnp.bfloat16)
                dv_part = jnp.dot(
                    p.astype(jnp.bfloat16), gc, preferred_element_type=jnp.float32
                )
                dk_part = jnp.dot(ds, qc, preferred_element_type=jnp.float32)
                dv_sum = dv_part if dv_sum is None else dv_sum + dv_part
                dk_sum = dk_part if dk_sum is None else dk_sum + dk_part
                dq[:, at] += jnp.dot(kt2, ds, preferred_element_type=jnp.float32)
            dk[j0] += dk_sum[:size]
            dv[j0] += dv_sum[:size]
            dk[j1] += dk_sum[size:]
            dv[j1] += dv_sum[size:]

        def put(dst, half):
            at = pl.ds(half * size, size)
            for head in range(heads):
                lanes = pl.ds(head * size, size)
                dst[at, lanes] = (dq[:, lanes].T * scale).astype(dst.dtype)

        for which in range(4):

            @pl.when(query == which)
            def _():
                put(dq_own if which < 2 else dq_sent, which % 2)

    for step in range(steps):
        for half in range(2):
            at = pl.ds(half * size, size)
            for dst, core in ((own_out[step], 0), (sent_out[step], 1)):
                block = step * 4 + core * 2 + half
                dst[at, pl.ds(0, size)] = (dk[block] * scale).astype(dst.dtype)
                dst[at, pl.ds(size, size)] = dv[block].astype(dst.dtype)


def per_device(queries, keys, values, out_grad, block_place):
    row_count, size = keys.shape
    block_len = row_count // 2
    heads = queries.shape[1] // size
    outer_size = lax.axis_size("outer")
    key_blocks = STEPS * 4
    scale = 1.0 / math.sqrt(size)
    inner = lax.axis_index("inner")
    outer = lax.axis_index("outer")
    where = jnp.stack([inner, outer, inner ^ 1, inner ^ 2]).astype(jnp.int32)

    kv = jnp.concatenate([keys, values], axis=1)
    q_far = swap(queries, "inner", 2)
    g_far = swap(out_grad, "inner", 2)
    own = [kv] + [from_behind(kv, "outer", step) for step in range(1, STEPS)]
    near = [swap(block, "inner", 1) for block in own]
    shards = [block for pair in zip(own, near) for block in pair]

    sizes = (heads, block_len, outer_size, key_blocks)
    smem = pl.BlockSpec(memory_space=pltpu.SMEM)
    vmem = pl.BlockSpec(memory_space=pltpu.VMEM)
    hbm = pl.BlockSpec(memory_space=pl.ANY)
    flops = 2 * 2 * block_len * heads * 4 * key_blocks * block_len * size
    common = [
        pltpu.VMEM((4, heads * block_len, size), jnp.bfloat16),
        pltpu.VMEM((4, heads * block_len, size), jnp.bfloat16),
        pltpu.VMEM((len(shards), row_count, 2 * size), jnp.bfloat16),
    ]
    tail = [
        pltpu.VMEM((3, block_len, block_len), jnp.float32),
        pltpu.SMEM((4, key_blocks + 1), jnp.int32),
        pltpu.SMEM((4,), jnp.int32),
        pltpu.SemaphoreType.DMA((len(shards),)),
    ]
    stats = pl.pallas_call(
        functools.partial(stats_kernel, sizes, scale),
        name="stats",
        out_shape=jax.ShapeDtypeStruct((4, 8, heads * block_len), jnp.float32),
        in_specs=[smem, smem] + [vmem] * 4 + [hbm] * len(shards),
        out_specs=vmem,
        scratch_shapes=common + tail,
        cost_estimate=pl.CostEstimate(flops=flops, bytes_accessed=1 << 21, transcendentals=0),
    )(block_place, where, queries, q_far, out_grad, g_far, *shards)
    other = swap(stats, "inner", 2)
    shard_f32 = jax.ShapeDtypeStruct((row_count, 2 * size), jnp.float32)
    shard_low = jax.ShapeDtypeStruct((row_count, 2 * size), jnp.bfloat16)
    got = pl.pallas_call(
        functools.partial(grads_kernel, sizes, scale),
        name="grads",
        out_shape=[
            jax.ShapeDtypeStruct(queries.shape, jnp.float32),
            jax.ShapeDtypeStruct(queries.shape, jnp.bfloat16),
        ]
        + [shard_f32] * STEPS
        + [shard_low] * STEPS,
        in_specs=[smem, smem] + [vmem] * 6 + [hbm] * len(shards),
        out_specs=[vmem] * (2 + 2 * STEPS),
        scratch_shapes=common
        + [
            pltpu.VMEM((key_blocks, block_len, block_len), jnp.bfloat16),
            pltpu.VMEM((key_blocks, block_len, size), jnp.float32),
            pltpu.VMEM((key_blocks, block_len, size), jnp.float32),
            pltpu.VMEM((size, heads * block_len), jnp.float32),
            pltpu.VMEM((4, 2, heads * block_len), jnp.float32),
        ]
        + tail,
        cost_estimate=pl.CostEstimate(flops=flops * 3, bytes_accessed=1 << 22, transcendentals=0),
    )(block_place, where, stats, other, queries, q_far, out_grad, g_far, *shards)
    dq_own, dq_sent = got[0], got[1]
    own_part, sent_part = got[2 : 2 + STEPS], got[2 + STEPS :]
    back = []
    for step in range(STEPS):
        whole = own_part[step] + swap(sent_part[step], "inner", 1).astype(jnp.float32)
        if step > 0:
            whole = from_behind(whole.astype(jnp.bfloat16), "outer", -step)
        back.append(whole.astype(jnp.float32))
    dq = dq_own + swap(dq_sent, "inner", 2).astype(jnp.float32)
    total = sum(back[1:], back[0]).astype(jnp.bfloat16)
    return dq.astype(jnp.bfloat16), total[:, :size], total[:, size:]


def solution(mesh):
    placed = (
        P(("inner", "outer"), None),
        P(("inner", "outer"), None),
        P(("inner", "outer"), None),
        P(("inner", "outer"), None),
        P(),
    )
    return jax.shard_map(
        per_device,
        mesh=mesh,
        in_specs=placed,
        out_specs=(
            P(("inner", "outer"), None),
            P(("inner", "outer"), None),
            P(("inner", "outer"), None),
        ),
        check_vma=False,
    )
```

```python
import functools
import math

import jax
import jax.numpy as jnp
from jax import lax
from jax.experimental import pallas as pl
from jax.experimental.pallas import tpu as pltpu
from jax.sharding import PartitionSpec as P


STEPS = 4
NEG = -1e30
LOG2E = math.log2(math.e)
NT = (((1,), (1,)), ((), ()))


def dot_nt(a, b):
    return lax.dot_general(a, b, NT, preferred_element_type=jnp.float32)


def from_behind(block, axis, distance):
    devices = range(lax.axis_size(axis))
    route = [((i - distance) % len(devices), i) for i in devices]
    return lax.ppermute(block, axis, route)


def swap(block, axis, bit):
    return lax.ppermute(block, axis, [(i, i ^ bit) for i in range(lax.axis_size(axis))])


def fill_bias(bias_ref):
    size = bias_ref.shape[1]
    key_off = lax.broadcasted_iota(jnp.int32, (size, size), 0)
    query_off = lax.broadcasted_iota(jnp.int32, (size, size), 1)
    bias_ref[0] = jnp.zeros((size, size), jnp.float32)
    bias_ref[1] = jnp.where(key_off <= query_off, 0.0, NEG).astype(jnp.float32)
    bias_ref[2] = jnp.full((size, size), NEG, jnp.float32)


def build_list(sizes, queries, blocks, place_ref, where_ref, list_ref):
    outer_size, key_blocks = sizes
    outer = where_ref[4]
    key_place = {}
    for block in blocks:
        step, core, half = block // 4, (block // 2) % 2, block % 2
        source = lax.rem(outer - step + outer_size, outer_size)
        key_place[block] = place_ref[(where_ref[core] * outer_size + source) * 2 + half]
    position = jnp.int32(0)
    for query in queries:
        query_place = place_ref[(where_ref[query // 2] * outer_size + outer) * 2 + query % 2]
        for block in blocks:
            kind = jnp.where(key_place[block] == query_place, 1, 0)
            list_ref[position] = (query * key_blocks + block) * 4 + kind
            position = position + jnp.where(key_place[block] <= query_place, 1, 0)
        list_ref[position] = (query * key_blocks + blocks[0]) * 4 + 2
        position = position + lax.rem(position, 2)
    for extra in range(4):
        list_ref[position + extra] = (queries[0] * key_blocks + blocks[0]) * 4 + 2
    return (position + 2) // 4


def entry_of(list_ref, index, key_blocks):
    e0, e1 = list_ref[2 * index], list_ref[2 * index + 1]
    at0, at1 = e0 // 4, e1 // 4
    return at0 // key_blocks, at0 % key_blocks, e0 % 4, at1 % key_blocks, e1 % 4


def score_tiles(entry, factor, qg, kv, bias, t_ref, dp_ref):
    query, j0, b0, j1, b1 = entry
    k2 = jnp.concatenate([kv[2 * j0], kv[2 * j1]], axis=0)
    v2 = jnp.concatenate([kv[2 * j0 + 1], kv[2 * j1 + 1]], axis=0)
    low, high = bias[b0], bias[b1]
    b2 = jnp.concatenate(
        [jnp.concatenate([low, low], axis=1), jnp.concatenate([high, high], axis=1)], axis=0
    )
    t_ref[...] = dot_nt(k2, qg[2 * query]) * factor + b2
    dp_ref[...] = dot_nt(v2, qg[2 * query + 1])


def stack_refs(refs, dst):
    for i, src in enumerate(refs):
        count = src.shape[0]
        dst[pl.ds(i * count, count)] = src[...]


def pair_loop(trips, load, use):
    load(0, 0)

    @pl.loop(0, trips)
    def _(i):
        load(2 * i + 1, 1)
        use(2 * i, 0)
        load(2 * i + 2, 0)
        use(2 * i + 1, 1)


def pack_kernel(where_ref, q_ref, g_ref, k_ref, v_ref, mine, theirs, kv):
    size = k_ref.shape[1]
    half_len = k_ref.shape[0] // 2
    pairs = q_ref.shape[1] // size // 2
    near = lax.rem(where_ref[0], 2)

    def put(dst, first):
        for half in range(2):
            for which, src in enumerate((q_ref, g_ref)):
                for head in range(pairs):
                    row = ((half * 2 + which) * pairs + head) * half_len
                    dst[pl.ds(row, half_len), :] = src[
                        pl.ds(half * half_len, half_len), pl.ds((first + head) * size, size)
                    ]

    for core in range(2):

        @pl.when(near == core)
        def _():
            put(mine, core * pairs)
            put(theirs, (1 - core) * pairs)

    for half in range(2):
        for which, src in enumerate((k_ref, v_ref)):
            kv[pl.ds((half * 2 + which) * half_len, half_len), :] = src[
                pl.ds(half * half_len, half_len), :
            ]


def stats_kernel(sizes, factor, which, shards, place_ref, where_ref, *rest):
    outer_size, key_blocks, _, width = sizes
    q_refs, kv_refs = rest[: len(which)], rest[len(which) : len(which) + shards]
    out_ref, qg, kv, bias, t0, d0, t1, d1, state, lists = rest[len(which) + shards :]
    stack_refs(kv_refs, kv)
    stack_refs(q_refs, qg)
    here = [2 * t + half for t in which for half in range(2)]
    first = here[0]
    trips = build_list(
        (outer_size, key_blocks), here, range(key_blocks), place_ref, where_ref, lists
    )
    fill_bias(bias)
    count = len(here)
    state[0] = jnp.full((count, 8, width), NEG, jnp.float32)
    state[1] = jnp.zeros((count, 8, width), jnp.float32)
    state[2] = jnp.zeros((count, 8, width), jnp.float32)
    slots = ((t0, d0), (t1, d1))

    def entry(n):
        query, j0, b0, j1, b1 = entry_of(lists, n, key_blocks)
        return query - first, j0, b0, j1, b1

    def load(n, slot):
        score_tiles(entry(n), factor, qg, kv, bias, *slots[slot])

    def use(n, slot):
        query = entry(n)[0]
        t_ref, d_ref = slots[slot]
        m, l, r = state[0, query], state[1, query], state[2, query]
        top = jnp.max(t_ref[...].reshape(-1, 8, width), axis=0)
        m_new = jnp.maximum(m, jnp.max(top, axis=0, keepdims=True))
        corr = jnp.exp2(m - m_new)
        p = jnp.exp2(t_ref[...].reshape(-1, 8, width) - m_new)
        state[0, query] = m_new
        state[1, query] = l * corr + jnp.sum(p, axis=0)
        state[2, query] = r * corr + jnp.sum(p * d_ref[...].reshape(-1, 8, width), axis=0)

    pair_loop(trips, load, use)
    for i in range(count):
        out_ref[i, 0:1] = state[0, i, 0:1]
        out_ref[i, 1:2] = jnp.sum(state[1, i], axis=0, keepdims=True)
        out_ref[i, 2:3] = jnp.sum(state[2, i], axis=0, keepdims=True)
        out_ref[i, 3:8] = jnp.zeros((5, width), jnp.float32)


def grads_kernel(sizes, scale, steps, last, place_ref, where_ref, *rest):
    outer_size, key_blocks, size, width = sizes
    pairs = width // size
    stat_refs = rest[:4] if not last else ()
    carry_in = rest[:2] if last else ()
    rest = rest[2:] if last else rest[4:]
    q_refs, kv_refs = rest[:4], rest[4 : 4 + 2 * len(steps)]
    rest = rest[4 + 2 * len(steps) :]
    outs, rest = rest[: 2 * len(steps)], rest[2 * len(steps) :]
    tops, rest = rest[: (4 if last else 2)], rest[(4 if last else 2) :]
    qg, kv, kt, dk, dv, dq, base, bias, t0, d0, t1, d1, lists = rest
    low = 4 * min(steps)
    blocks = [4 * step + i for step in sorted(steps) for i in range(4)]
    stack_refs(kv_refs, kv)
    stack_refs(q_refs, qg)
    if last:
        dq[...] = carry_in[0][...]
        base[...] = carry_in[1][...]
    trips = build_list((outer_size, key_blocks), range(8), blocks, place_ref, where_ref, lists)
    fill_bias(bias)
    if not last:
        for query in range(8):
            a = stat_refs[query // 4][query % 4]
            b = stat_refs[2 + (1 - query // 4)][query % 4]
            m = jnp.maximum(a[0:1], b[0:1])
            ea, eb = jnp.exp2(a[0:1] - m), jnp.exp2(b[0:1] - m)
            total = a[1:2] * ea + b[1:2] * eb
            base[query, 0:1] = m + jnp.log2(total)
            base[query, 1:2] = (a[2:3] * ea + b[2:3] * eb) / total
            base[query, 2:8] = jnp.zeros((6, width), jnp.float32)
        dq[...] = jnp.zeros_like(dq)
    dk[...] = jnp.zeros_like(dk)
    dv[...] = jnp.zeros_like(dv)
    for block in range(len(blocks)):
        kt[block] = kv[2 * block].T
    factor = scale * LOG2E
    slots = ((t0, d0), (t1, d1))

    def entry(n):
        query, j0, b0, j1, b1 = entry_of(lists, n, key_blocks)
        return query, j0 - low, b0, j1 - low, b1

    def load(n, slot):
        score_tiles(entry(n), factor, qg, kv, bias, *slots[slot])

    def use(n, slot):
        query, j0, _, j1, _ = entry(n)
        t_ref, d_ref = slots[slot]
        p = jnp.exp2(t_ref[...] - base[query, 0:1])
        ds = (p * (d_ref[...] - base[query, 1:2])).astype(jnp.bfloat16)
        p = p.astype(jnp.bfloat16)
        dv_part = jnp.dot(p, qg[2 * query + 1], preferred_element_type=jnp.float32)
        dk_part = jnp.dot(ds, qg[2 * query], preferred_element_type=jnp.float32)
        kt2 = jnp.concatenate([kt[j0], kt[j1]], axis=1)
        dq[query] += jnp.dot(kt2, ds, preferred_element_type=jnp.float32)
        dk[j0] += dk_part[:size]
        dv[j0] += dv_part[:size]
        dk[j1] += dk_part[size:]
        dv[j1] += dv_part[size:]

    pair_loop(trips, load, use)
    for i in range(len(steps)):
        for half in range(2):
            for core in range(2):
                dst = outs[2 * i + core]
                block = i * 4 + core * 2 + half
                dst[pl.ds(2 * half * size, size), :] = (dk[block] * scale).astype(dst.dtype)
                dst[pl.ds((2 * half + 1) * size, size), :] = dv[block].astype(dst.dtype)
    if last:
        for query in range(8):
            dst = tops[query // 2]
            for head in range(pairs):
                dst[pl.ds((query % 2) * size, size), pl.ds(head * size, size)] = (
                    dq[query, :, pl.ds(head * size, size)].T * scale
                ).astype(dst.dtype)
    else:
        tops[0][...] = dq[...]
        tops[1][...] = base[...]


def attention_grads(queries, keys, values, out_grad, block_place):
    row_count, size = keys.shape
    block_len = row_count // 2
    pairs = queries.shape[1] // size // 2
    width = pairs * block_len
    outer_size = lax.axis_size("outer")
    key_blocks = STEPS * 4
    scale = 1.0 / math.sqrt(size)
    inner = lax.axis_index("inner")
    outer = lax.axis_index("outer")
    where = jnp.stack([inner, inner ^ 1, inner ^ 2, inner ^ 3, outer]).astype(jnp.int32)
    smem = pl.BlockSpec(memory_space=pltpu.SMEM)
    vmem = pl.BlockSpec(memory_space=pltpu.VMEM)
    params = pltpu.CompilerParams(vmem_limit_bytes=16 << 20)
    low, full = jnp.bfloat16, jnp.float32

    q_shape, kv_shape = (4 * width, size), (4 * block_len, size)
    mine, theirs, kv = pl.pallas_call(
        pack_kernel,
        name="pack",
        out_shape=[
            jax.ShapeDtypeStruct(q_shape, low),
            jax.ShapeDtypeStruct(q_shape, low),
            jax.ShapeDtypeStruct(kv_shape, low),
        ],
        in_specs=[smem] + [vmem] * 4,
        out_specs=[vmem] * 3,
        compiler_params=params,
    )(where, queries, out_grad, keys, values)
    asked = [mine, swap(theirs, "inner", 1), swap(mine, "inner", 2), swap(theirs, "inner", 3)]
    own = [kv] + [from_behind(kv, "outer", step) for step in range(1, STEPS)]
    near = [swap(block, "inner", 1) for block in own]
    q_parts = [part.reshape(4, width, size) for part in asked]
    shards = [block.reshape(4, block_len, size) for two in zip(own, near) for block in two]

    sizes = (outer_size, key_blocks, size, width)
    flops = 2 * 2 * width * 8 * key_blocks * block_len * size
    tile = pltpu.VMEM((2 * block_len, width), full)
    bias_table = pltpu.VMEM((3, block_len, block_len), full)

    def stats_call(which):
        count = 2 * len(which)
        return pl.pallas_call(
            functools.partial(stats_kernel, sizes, scale * LOG2E, which, len(shards)),
            name="stats",
            out_shape=jax.ShapeDtypeStruct((count, 8, width), full),
            in_specs=[smem, smem] + [vmem] * (len(which) + len(shards)),
            out_specs=vmem,
            scratch_shapes=[
                pltpu.VMEM((2 * count, width, size), low),
                pltpu.VMEM((2 * key_blocks, block_len, size), low),
                bias_table,
                tile,
                tile,
                tile,
                tile,
                pltpu.VMEM((3, count, 8, width), full),
                pltpu.SMEM((count * (key_blocks + 1) + 8,), jnp.int32),
            ],
            compiler_params=params,
            cost_estimate=pl.CostEstimate(
                flops=flops // 2, bytes_accessed=1 << 20, transcendentals=0
            ),
        )(block_place, where, *[q_parts[t] for t in which], *shards)

    stats = []
    for which in ((0, 1), (2, 3)):
        stats.append(stats_call(which))
    others = [swap(stat, "inner", 2) for stat in stats]
    shard_f32 = jax.ShapeDtypeStruct(kv_shape, full)
    shard_low = jax.ShapeDtypeStruct(kv_shape, low)

    def grads_call(steps, last, *extra):
        n = len(steps)
        if last:
            tops = [jax.ShapeDtypeStruct((row_count, width), full if t == 0 else low) for t in range(4)]
        else:
            tops = [
                jax.ShapeDtypeStruct((8, size, width), full),
                jax.ShapeDtypeStruct((8, 8, width), full),
            ]
        used = [part for step in steps for part in shards[2 * step : 2 * step + 2]]
        return pl.pallas_call(
            functools.partial(grads_kernel, sizes, scale, steps, last),
            name="grads",
            out_shape=[shard_f32, shard_low] * n + tops,
            in_specs=[smem, smem] + [vmem] * (len(extra) + 4 + 2 * n),
            out_specs=[vmem] * (2 * n + len(tops)),
            scratch_shapes=[
                pltpu.VMEM((16, width, size), low),
                pltpu.VMEM((8 * n, block_len, size), low),
                pltpu.VMEM((4 * n, size, block_len), low),
                pltpu.VMEM((4 * n, block_len, size), full),
                pltpu.VMEM((4 * n, block_len, size), full),
                pltpu.VMEM((8, size, width), full),
                pltpu.VMEM((8, 8, width), full),
                bias_table,
                tile,
                tile,
                tile,
                tile,
                pltpu.SMEM((8 * (4 * n + 1) + 8,), jnp.int32),
            ],
            compiler_params=params,
            cost_estimate=pl.CostEstimate(
                flops=flops * 3 * n // STEPS, bytes_accessed=1 << 21, transcendentals=0
            ),
        )(block_place, where, *extra, *q_parts, *used)

    far_steps = tuple(range(STEPS // 2, STEPS))
    near_steps = tuple(range(STEPS // 2))
    parts = {}
    got = grads_call(far_steps, False, *stats, *others)
    for i, step in enumerate(far_steps):
        parts[step] = got[2 * i : 2 * i + 2]
    got = grads_call(near_steps, True, *got[2 * len(far_steps) :])
    for i, step in enumerate(near_steps):
        parts[step] = got[2 * i : 2 * i + 2]
    tops = got[2 * len(near_steps) :]
    back = []
    for step in reversed(range(STEPS)):
        whole = parts[step][0] + swap(parts[step][1], "inner", 1).astype(full)
        if step > 0:
            whole = from_behind(whole.astype(low), "outer", -step)
        back.append(whole.astype(full))
    heads_mine = tops[0] + swap(tops[2], "inner", 2).astype(full)
    heads_other = swap(tops[1], "inner", 1).astype(full) + swap(tops[3], "inner", 3).astype(full)
    first = inner % 2 == 0
    dq = jnp.concatenate(
        [jnp.where(first, heads_mine, heads_other), jnp.where(first, heads_other, heads_mine)], axis=1
    )
    total = sum(back[1:], back[0]).astype(low).reshape(2, 2, block_len, size)
    return (
        dq.astype(low),
        total[:, 0].reshape(row_count, size),
        total[:, 1].reshape(row_count, size),
    )


def solution(mesh):
    placed = (
        P(("inner", "outer"), None),
        P(("inner", "outer"), None),
        P(("inner", "outer"), None),
        P(("inner", "outer"), None),
        P(),
    )
    return jax.shard_map(
        attention_grads,
        mesh=mesh,
        in_specs=placed,
        out_specs=(
            P(("inner", "outer"), None),
            P(("inner", "outer"), None),
            P(("inner", "outer"), None),
        ),
        check_vma=False,
    )
```

```python
import functools
import math

import jax
import jax.numpy as jnp
from jax import lax
from jax.experimental import pallas as pl
from jax.experimental.pallas import tpu as pltpu
from jax.sharding import PartitionSpec as P


STEPS = 4
NEG = -1e30
LOG2E = math.log2(math.e)
NT = (((1,), (1,)), ((), ()))


def dot_nt(a, b):
    return lax.dot_general(a, b, NT, preferred_element_type=jnp.float32)


def from_behind(block, axis, distance):
    devices = range(lax.axis_size(axis))
    route = [((i - distance) % len(devices), i) for i in devices]
    return lax.ppermute(block, axis, route)


def swap(block, axis, bit):
    return lax.ppermute(block, axis, [(i, i ^ bit) for i in range(lax.axis_size(axis))])


def fill_bias(bias_ref):
    size = bias_ref.shape[1]
    key_off = lax.broadcasted_iota(jnp.int32, (size, size), 0)
    query_off = lax.broadcasted_iota(jnp.int32, (size, size), 1)
    bias_ref[0] = jnp.zeros((size, size), jnp.float32)
    bias_ref[1] = jnp.where(key_off <= query_off, 0.0, NEG).astype(jnp.float32)
    bias_ref[2] = jnp.full((size, size), NEG, jnp.float32)


def build_list(sizes, queries, blocks, where_ref, list_ref):
    outer_size, key_blocks = sizes
    outer = where_ref[4]
    key_place = {}
    for block in blocks:
        step, core, half = block // 4, (block // 2) % 2, block % 2
        source = lax.rem(outer - step + outer_size, outer_size)
        key_place[block] = where_ref[8 + (where_ref[core] * outer_size + source) * 2 + half]
    position = jnp.int32(0)
    for query in queries:
        query_place = where_ref[8 + (where_ref[query // 2] * outer_size + outer) * 2 + query % 2]
        for block in blocks:
            kind = jnp.where(key_place[block] == query_place, 1, 0)
            list_ref[position] = (query * key_blocks + block) * 4 + kind
            position = position + jnp.where(key_place[block] <= query_place, 1, 0)
        list_ref[position] = (query * key_blocks + blocks[0]) * 4 + 2
        position = position + lax.rem(position, 2)
    for extra in range(10):
        list_ref[position + extra] = (queries[0] * key_blocks + blocks[0]) * 4 + 2
    return (position + 6) // 8


def entry_of(list_ref, index, key_blocks):
    e0, e1 = list_ref[2 * index], list_ref[2 * index + 1]
    at0, at1 = e0 // 4, e1 // 4
    return at0 // key_blocks, at0 % key_blocks, e0 % 4, at1 % key_blocks, e1 % 4


def score_tiles(entry, factor, qg, kv, bias, t_ref, dp_ref, top_ref=None):
    query, j0, b0, j1, b1 = entry
    k2 = jnp.concatenate([kv[2 * j0], kv[2 * j1]], axis=0)
    v2 = jnp.concatenate([kv[2 * j0 + 1], kv[2 * j1 + 1]], axis=0)
    low, high = bias[b0], bias[b1]
    b2 = jnp.concatenate(
        [jnp.concatenate([low, low], axis=1), jnp.concatenate([high, high], axis=1)], axis=0
    )
    t = dot_nt(k2, qg[2 * query]) * factor + b2
    t_ref[...] = t
    if top_ref is not None:
        top_ref[...] = jnp.max(t.reshape(-1, 8, t.shape[1]), axis=0)
    dp_ref[...] = dot_nt(v2, qg[2 * query + 1])


def stack_refs(refs, dst):
    for i, src in enumerate(refs):
        count = src.shape[0]
        dst[pl.ds(i * count, count)] = src[...]


def pair_loop(trips, load, use):
    load(0, 0)
    load(1, 1)

    @pl.loop(0, trips)
    def _(i):
        load(4 * i + 2, 2)
        load(4 * i + 3, 3)
        use(4 * i, 0)
        use(4 * i + 1, 1)
        load(4 * i + 4, 0)
        load(4 * i + 5, 1)
        use(4 * i + 2, 2)
        use(4 * i + 3, 3)


def pack_kernel(size, where_ref, q_ref, g_ref, mine, theirs, sems):
    half_len = q_ref.shape[0] // 2
    pairs = q_ref.shape[1] // size // 2
    near = lax.rem(where_ref[0], 2)
    copies = []

    def put(src, dst):
        copies.append(pltpu.make_async_copy(src, dst, sems.at[len(copies)]))

    for half in range(2):
        rows = pl.ds(half * half_len, half_len)
        for dst, core in ((mine, near), (theirs, 1 - near)):
            for which, src in enumerate((q_ref, g_ref)):
                for head in range(pairs):
                    row = ((half * 2 + which) * pairs + head) * half_len
                    lane = pl.multiple_of((core * pairs + head) * size, size)
                    put(src.at[rows, pl.ds(lane, size)], dst.at[pl.ds(row, half_len), :])
    for copy in copies:
        copy.start()
    for copy in copies:
        copy.wait()


def stats_kernel(sizes, factor, which, shards, where_ref, *rest):
    outer_size, key_blocks, _, width = sizes
    merged = which[0] > 0
    if merged:
        early, rest = rest[0], rest[1:]
    q_refs, kv_refs = rest[: len(which)], rest[len(which) : len(which) + shards]
    out_ref, qg, kv, bias, *tiles, state, lists = rest[len(which) + shards :]
    stack_refs(kv_refs, kv)
    stack_refs(q_refs, qg)
    here = [2 * t + half for t in which for half in range(2)]
    first = here[0]
    trips = build_list(
        (outer_size, key_blocks), here, range(key_blocks), where_ref, lists
    )
    fill_bias(bias)
    count = len(here)
    state[0] = jnp.full((count, 8, width), NEG, jnp.float32)
    state[1] = jnp.zeros((count, 8, width), jnp.float32)
    state[2] = jnp.zeros((count, 8, width), jnp.float32)
    slots = [tiles[3 * i : 3 * i + 3] for i in range(4)]

    def entry(n):
        query, j0, b0, j1, b1 = entry_of(lists, n, key_blocks)
        return query - first, j0, b0, j1, b1

    def load(n, slot):
        score_tiles(entry(n), factor, qg, kv, bias, *slots[slot])

    def use(n, slot):
        query = entry(n)[0]
        t_ref, d_ref, top = slots[slot]
        m, l, r = state[0, query], state[1, query], state[2, query]
        m_new = jnp.maximum(m, jnp.max(top[...], axis=0, keepdims=True))
        corr = jnp.exp2(m - m_new)
        p = jnp.exp2(t_ref[...].reshape(-1, 8, width) - m_new)
        state[0, query] = m_new
        state[1, query] = l * corr + jnp.sum(p, axis=0)
        state[2, query] = r * corr + jnp.sum(p * d_ref[...].reshape(-1, 8, width), axis=0)

    pair_loop(trips, load, use)
    for i in range(count):
        at = pl.ds(first + i if merged else i, 1)
        out_ref[0, at] = state[0, i, 0:1]
        out_ref[1, at] = jnp.sum(state[1, i], axis=0, keepdims=True)
        out_ref[2, at] = jnp.sum(state[2, i], axis=0, keepdims=True)
    if merged:
        out_ref[:, pl.ds(0, first)] = early[:, pl.ds(0, first)]
    else:
        out_ref[:, pl.ds(count, count)] = jnp.zeros((3, count, width), jnp.float32)


def grads_kernel(sizes, scale, steps, last, where_ref, *rest):
    outer_size, key_blocks, size, width = sizes
    pairs = width // size
    carry_in, rest = rest[:2], rest[2:]
    q_refs, kv_refs = rest[:4], rest[4 : 4 + 2 * len(steps)]
    rest = rest[4 + 2 * len(steps) :]
    outs, rest = rest[: 2 * len(steps)], rest[2 * len(steps) :]
    tops, rest = rest[: (4 if last else 2)], rest[(4 if last else 2) :]
    qg, kv, kt, dk, dv, dq, base, bias, *tiles, lists = rest
    low = 4 * min(steps)
    blocks = [4 * step + i for step in sorted(steps) for i in range(4)]
    stack_refs(kv_refs, kv)
    stack_refs(q_refs, qg)
    if last:
        dq[...] = carry_in[0][...]
        base[...] = carry_in[1][...]
    trips = build_list((outer_size, key_blocks), range(8), blocks, where_ref, lists)
    fill_bias(bias)
    if not last:
        for query in range(8):
            here, there = pl.ds(query, 1), pl.ds(query ^ 4, 1)
            mine, other = carry_in
            m = jnp.maximum(mine[0, here], other[0, there])
            ea, eb = jnp.exp2(mine[0, here] - m), jnp.exp2(other[0, there] - m)
            total = mine[1, here] * ea + other[1, there] * eb
            base[query, 0:1] = m + jnp.log2(total)
            base[query, 1:2] = (mine[2, here] * ea + other[2, there] * eb) / total
            base[query, 2:8] = jnp.zeros((6, width), jnp.float32)
        dq[...] = jnp.zeros_like(dq)
    dk[...] = jnp.zeros_like(dk)
    dv[...] = jnp.zeros_like(dv)
    for block in range(len(blocks)):
        kt[block] = kv[2 * block].T
    factor = scale * LOG2E
    slots = [tiles[2 * i : 2 * i + 2] for i in range(4)]

    def entry(n):
        query, j0, b0, j1, b1 = entry_of(lists, n, key_blocks)
        return query, j0 - low, b0, j1 - low, b1

    def load(n, slot):
        score_tiles(entry(n), factor, qg, kv, bias, *slots[slot])

    def use(n, slot):
        query, j0, _, j1, _ = entry(n)
        t_ref, d_ref = slots[slot]
        p = jnp.exp2(t_ref[...] - base[query, 0:1])
        ds = (p * (d_ref[...] - base[query, 1:2])).astype(jnp.bfloat16)
        p = p.astype(jnp.bfloat16)
        dv_part = jnp.dot(p, qg[2 * query + 1], preferred_element_type=jnp.float32)
        dk_part = jnp.dot(ds, qg[2 * query], preferred_element_type=jnp.float32)
        kt2 = jnp.concatenate([kt[j0], kt[j1]], axis=1)
        dq[query] += jnp.dot(kt2, ds, preferred_element_type=jnp.float32)
        dk[j0] += dk_part[:size]
        dv[j0] += dv_part[:size]
        dk[j1] += dk_part[size:]
        dv[j1] += dv_part[size:]

    pair_loop(trips, load, use)
    for i in range(len(steps)):
        for half in range(2):
            for core in range(2):
                dst = outs[2 * i + core]
                block = i * 4 + core * 2 + half
                dst[pl.ds(2 * half * size, size), :] = (dk[block] * scale).astype(dst.dtype)
                dst[pl.ds((2 * half + 1) * size, size), :] = dv[block].astype(dst.dtype)
    if last:
        for query in range(8):
            dst = tops[query // 2]
            for head in range(pairs):
                dst[pl.ds((query % 2) * size, size), pl.ds(head * size, size)] = (
                    dq[query, :, pl.ds(head * size, size)].T * scale
                ).astype(dst.dtype)
    else:
        tops[0][...] = dq[...]
        tops[1][...] = base[...]


def attention_grads(queries, keys, values, out_grad, block_place):
    row_count, size = keys.shape
    block_len = row_count // 2
    pairs = queries.shape[1] // size // 2
    width = pairs * block_len
    outer_size = lax.axis_size("outer")
    key_blocks = STEPS * 4
    scale = 1.0 / math.sqrt(size)
    inner = lax.axis_index("inner")
    outer = lax.axis_index("outer")
    where = jnp.concatenate(
        [jnp.stack([inner, inner ^ 1, inner ^ 2, inner ^ 3, outer] + [outer] * 3), block_place]
    )
    smem = pl.BlockSpec(memory_space=pltpu.SMEM)
    vmem = pl.BlockSpec(memory_space=pltpu.VMEM)
    params = pltpu.CompilerParams(vmem_limit_bytes=16 << 20)
    low, full = jnp.bfloat16, jnp.float32

    q_shape, kv_shape = (4 * width, size), (4 * block_len, size)
    kv = jnp.stack(
        [keys.reshape(2, block_len, size), values.reshape(2, block_len, size)], axis=1
    ).reshape(kv_shape)
    own2 = from_behind(kv, "outer", 2)
    mine, theirs = pl.pallas_call(
        functools.partial(pack_kernel, size),
        name="pack",
        out_shape=[jax.ShapeDtypeStruct(q_shape, low)] * 2,
        in_specs=[smem] + [pl.BlockSpec(memory_space=pltpu.HBM)] * 2,
        out_specs=[vmem] * 2,
        scratch_shapes=[pltpu.SemaphoreType.DMA((8 * pairs,))],
        compiler_params=params,
    )(where, queries, out_grad)
    asked = [mine, swap(theirs, "inner", 1), swap(mine, "inner", 2), swap(theirs, "inner", 3)]
    own1 = swap(jnp.where(outer % 2 == 1, own2, kv), "outer", 1)
    own3 = from_behind(own2, "outer", 1)
    own = [kv, own1, own2, own3]
    near = [swap(block, "inner", 1) for block in own]
    q_parts = [part.reshape(4, width, size) for part in asked]
    shards = [block.reshape(4, block_len, size) for two in zip(own, near) for block in two]

    sizes = (outer_size, key_blocks, size, width)
    flops = 2 * 2 * width * 8 * key_blocks * block_len * size
    tile = pltpu.VMEM((2 * block_len, width), full)
    bias_table = pltpu.VMEM((3, block_len, block_len), full)

    def stats_call(which, *early):
        count = 2 * len(which)
        return pl.pallas_call(
            functools.partial(stats_kernel, sizes, scale * LOG2E, which, len(shards)),
            name="stats",
            out_shape=jax.ShapeDtypeStruct((3, 8, width), full),
            in_specs=[smem] + [vmem] * (len(early) + len(which) + len(shards)),
            out_specs=vmem,
            scratch_shapes=[
                pltpu.VMEM((2 * count, width, size), low),
                pltpu.VMEM((2 * key_blocks, block_len, size), low),
                bias_table,
                *[tile, tile, pltpu.VMEM((8, width), full)] * 4,
                pltpu.VMEM((3, count, 8, width), full),
                pltpu.SMEM((count * key_blocks + 16,), jnp.int32),
            ],
            compiler_params=params,
            cost_estimate=pl.CostEstimate(
                flops=flops // 2, bytes_accessed=1 << 20, transcendentals=0
            ),
        )(where, *early, *[q_parts[t] for t in which], *shards)

    early = stats_call((0, 1))
    stats = stats_call((2, 3), early)
    others = swap(stats, "inner", 2)
    shard_f32 = jax.ShapeDtypeStruct(kv_shape, full)
    shard_low = jax.ShapeDtypeStruct(kv_shape, low)

    def grads_call(steps, last, *extra):
        n = len(steps)
        if last:
            tops = [jax.ShapeDtypeStruct((row_count, width), full if t == 0 else low) for t in range(4)]
        else:
            tops = [
                jax.ShapeDtypeStruct((8, size, width), full),
                jax.ShapeDtypeStruct((8, 8, width), full),
            ]
        used = [part for step in steps for part in shards[2 * step : 2 * step + 2]]
        return pl.pallas_call(
            functools.partial(grads_kernel, sizes, scale, steps, last),
            name="grads",
            out_shape=[shard_f32, shard_low] * n + tops,
            in_specs=[smem] + [vmem] * (len(extra) + 4 + 2 * n),
            out_specs=[vmem] * (2 * n + len(tops)),
            scratch_shapes=[
                pltpu.VMEM((16, width, size), low),
                pltpu.VMEM((8 * n, block_len, size), low),
                pltpu.VMEM((4 * n, size, block_len), low),
                pltpu.VMEM((4 * n, block_len, size), full),
                pltpu.VMEM((4 * n, block_len, size), full),
                pltpu.VMEM((8, size, width), full),
                pltpu.VMEM((8, 8, width), full),
                bias_table,
                *[tile] * 8,
                pltpu.SMEM((8 * 4 * n + 16,), jnp.int32),
            ],
            compiler_params=params,
            cost_estimate=pl.CostEstimate(
                flops=flops * 3 * n // STEPS, bytes_accessed=1 << 21, transcendentals=0
            ),
        )(where, *extra, *q_parts, *used)

    far_steps = tuple(range(STEPS // 2, STEPS))
    near_steps = tuple(range(STEPS // 2))
    parts = {}
    got = grads_call(far_steps, False, stats, others)
    for i, step in enumerate(far_steps):
        parts[step] = got[2 * i : 2 * i + 2]
    got = grads_call(near_steps, True, *got[2 * len(far_steps) :])
    for i, step in enumerate(near_steps):
        parts[step] = got[2 * i : 2 * i + 2]
    tops = got[2 * len(near_steps) :]
    back = []
    for step in reversed(range(STEPS)):
        whole = parts[step][0] + swap(parts[step][1], "inner", 1).astype(full)
        if step > 0:
            whole = from_behind(whole.astype(low), "outer", -step)
        back.append(whole.astype(full))
    heads_mine = tops[0] + swap(tops[2], "inner", 2).astype(full)
    heads_other = swap(tops[1], "inner", 1).astype(full) + swap(tops[3], "inner", 3).astype(full)
    first = inner % 2 == 0
    dq = jnp.concatenate(
        [jnp.where(first, heads_mine, heads_other), jnp.where(first, heads_other, heads_mine)], axis=1
    )
    total = sum(back[1:], back[0]).astype(low).reshape(2, 2, block_len, size)
    return (
        dq.astype(low),
        total[:, 0].reshape(row_count, size),
        total[:, 1].reshape(row_count, size),
    )


def solution(mesh):
    placed = (
        P(("inner", "outer"), None),
        P(("inner", "outer"), None),
        P(("inner", "outer"), None),
        P(("inner", "outer"), None),
        P(),
    )
    return jax.shard_map(
        attention_grads,
        mesh=mesh,
        in_specs=placed,
        out_specs=(
            P(("inner", "outer"), None),
            P(("inner", "outer"), None),
            P(("inner", "outer"), None),
        ),
        check_vma=False,
    )
```

```python
import functools
import math

import jax
import jax.numpy as jnp
from jax import lax
from jax.experimental import pallas as pl
from jax.experimental.pallas import tpu as pltpu
from jax.sharding import PartitionSpec as P


STEPS = 4
NEG = -1e30
LOG2E = math.log2(math.e)
NT = (((1,), (1,)), ((), ()))


def dot_nt(a, b):
    return lax.dot_general(a, b, NT, preferred_element_type=jnp.float32)


def from_behind(block, axis, distance):
    devices = range(lax.axis_size(axis))
    route = [((i - distance) % len(devices), i) for i in devices]
    return lax.ppermute(block, axis, route)


def swap(block, axis, bit):
    return lax.ppermute(block, axis, [(i, i ^ bit) for i in range(lax.axis_size(axis))])


def fill_bias(bias_ref):
    size = bias_ref.shape[1]
    key_off = lax.broadcasted_iota(jnp.int32, (size, size), 0)
    query_off = lax.broadcasted_iota(jnp.int32, (size, size), 1)
    bias_ref[0] = jnp.zeros((size, size), jnp.float32)
    bias_ref[1] = jnp.where(key_off <= query_off, 0.0, NEG).astype(jnp.float32)
    bias_ref[2] = jnp.full((size, size), NEG, jnp.float32)


def build_list(sizes, plan, where_ref, list_ref):
    outer_size, key_blocks = sizes
    outer = where_ref[4]
    key_place = {}
    for block in sorted({block for _, blocks in plan for block in blocks}):
        step, core, half = block // 4, (block // 2) % 2, block % 2
        source = lax.rem(outer - step + outer_size, outer_size)
        key_place[block] = where_ref[8 + (where_ref[core] * outer_size + source) * 2 + half]
    position = jnp.int32(0)
    pad = (plan[0][0] * key_blocks + plan[0][1][0]) * 4 + 2
    for query, blocks in plan:
        query_place = where_ref[8 + (where_ref[query // 2] * outer_size + outer) * 2 + query % 2]
        for block in blocks:
            kind = jnp.where(key_place[block] == query_place, 1, 0)
            list_ref[position] = (query * key_blocks + block) * 4 + kind
            position = position + jnp.where(key_place[block] <= query_place, 1, 0)
        list_ref[position] = (query * key_blocks + blocks[0]) * 4 + 2
        position = position + lax.rem(position, 2)
    for extra in range(10):
        list_ref[position + extra] = pad
    return (position + 6) // 8


def blocks_of(steps):
    return [4 * step + i for step in steps for i in range(4)]


def entry_of(list_ref, index, key_blocks):
    e0, e1 = list_ref[2 * index], list_ref[2 * index + 1]
    at0, at1 = e0 // 4, e1 // 4
    return at0 // key_blocks, at0 % key_blocks, e0 % 4, at1 % key_blocks, e1 % 4


def score_tiles(entry, factor, qg, kv, bias, t_ref, dp_ref, top_ref=None):
    query, j0, b0, j1, b1 = entry
    k2 = jnp.concatenate([kv[2 * j0], kv[2 * j1]], axis=0)
    v2 = jnp.concatenate([kv[2 * j0 + 1], kv[2 * j1 + 1]], axis=0)
    low, high = bias[b0], bias[b1]
    b2 = jnp.concatenate(
        [jnp.concatenate([low, low], axis=1), jnp.concatenate([high, high], axis=1)], axis=0
    )
    t = dot_nt(k2, qg[2 * query]) * factor + b2
    t_ref[...] = t
    if top_ref is not None:
        top_ref[...] = jnp.max(t.reshape(-1, 8, t.shape[1]), axis=0)
    dp_ref[...] = dot_nt(v2, qg[2 * query + 1])


def stack_refs(refs, dst):
    for i, src in enumerate(refs):
        count = src.shape[0]
        dst[pl.ds(i * count, count)] = src[...]


def pair_loop(trips, load, use):
    load(0, 0)
    load(1, 1)

    @pl.loop(0, trips)
    def _(i):
        load(4 * i + 2, 2)
        load(4 * i + 3, 3)
        use(4 * i, 0)
        use(4 * i + 1, 1)
        load(4 * i + 4, 0)
        load(4 * i + 5, 1)
        use(4 * i + 2, 2)
        use(4 * i + 3, 3)


def stats_kernel(sizes, factor, steps, merged, where_ref, *rest):
    outer_size, key_blocks, _, width = sizes
    if merged:
        early, rest = rest[0], rest[1:]
    count = 8 if merged else 4
    held = list(range(STEPS)) if merged else list(steps)
    q_refs, kv_refs = rest[: count // 2], rest[count // 2 : count // 2 + 2 * len(held)]
    out_ref, qg, kv, bias, *tiles, state, lists = rest[count // 2 + 2 * len(held) :]
    stack_refs(kv_refs, kv)
    stack_refs(q_refs, qg)
    plan = [
        (query, blocks_of(held if query >= 4 else steps))
        for query in (list(range(4, 8)) if merged else []) + list(range(4))
    ]
    trips = build_list((outer_size, key_blocks), plan, where_ref, lists)
    fill_bias(bias)
    state[0] = jnp.full((count, 8, width), NEG, jnp.float32)
    state[1] = jnp.zeros((count, 8, width), jnp.float32)
    state[2] = jnp.zeros((count, 8, width), jnp.float32)
    if merged:
        for i in range(4):
            at = pl.ds(i, 1)
            state[0, i] = jnp.broadcast_to(early[0, at], (8, width))
            state[1, i, 0:1] = early[1, at]
            state[2, i, 0:1] = early[2, at]
    gap = held[1] - held[0]
    slots = [tiles[3 * i : 3 * i + 3] for i in range(4)]

    def slot_of(block):
        return block if gap == 1 else (block // 4 // gap) * 4 + block % 4

    def entry(n):
        query, j0, b0, j1, b1 = entry_of(lists, n, key_blocks)
        return query, slot_of(j0), b0, slot_of(j1), b1

    def load(n, slot):
        score_tiles(entry(n), factor, qg, kv, bias, *slots[slot])

    def use(n, slot):
        query = entry(n)[0]
        t_ref, d_ref, top = slots[slot]
        m, l, r = state[0, query], state[1, query], state[2, query]
        m_new = jnp.maximum(m, jnp.max(top[...], axis=0, keepdims=True))
        corr = jnp.exp2(m - m_new)
        p = jnp.exp2(t_ref[...].reshape(-1, 8, width) - m_new)
        state[0, query] = m_new
        state[1, query] = l * corr + jnp.sum(p, axis=0)
        state[2, query] = r * corr + jnp.sum(p * d_ref[...].reshape(-1, 8, width), axis=0)

    pair_loop(trips, load, use)
    for i in range(count):
        at = pl.ds(i, 1)
        out_ref[0, at] = state[0, i, 0:1]
        out_ref[1, at] = jnp.sum(state[1, i], axis=0, keepdims=True)
        out_ref[2, at] = jnp.sum(state[2, i], axis=0, keepdims=True)
    if not merged:
        out_ref[:, pl.ds(count, count)] = jnp.zeros((3, count, width), jnp.float32)


def grads_kernel(sizes, scale, steps, last, where_ref, *rest):
    outer_size, key_blocks, size, width = sizes
    pairs = width // size
    carry_in, rest = rest[:2], rest[2:]
    q_refs, kv_refs = rest[:4], rest[4 : 4 + 2 * len(steps)]
    rest = rest[4 + 2 * len(steps) :]
    outs, sent, rest = rest[: len(steps)], rest[len(steps)], rest[len(steps) + 1 :]
    tops, rest = rest[: (3 if last else 2)], rest[(3 if last else 2) :]
    qg, kv, kt, dk, dv, dq, base, bias, *tiles, lists = rest
    low = 4 * min(steps)
    blocks = blocks_of(steps)
    stack_refs(kv_refs, kv)
    stack_refs(q_refs, qg)
    if last:
        dq[...] = carry_in[0][...]
        base[...] = carry_in[1][...]
    plan = [(query, blocks) for query in range(8)]
    trips = build_list((outer_size, key_blocks), plan, where_ref, lists)
    fill_bias(bias)
    if not last:
        for query in range(8):
            here, there = pl.ds(query, 1), pl.ds(query ^ 4, 1)
            mine, other = carry_in
            m = jnp.maximum(mine[0, here], other[0, there])
            ea, eb = jnp.exp2(mine[0, here] - m), jnp.exp2(other[0, there] - m)
            total = mine[1, here] * ea + other[1, there] * eb
            base[query, 0:1] = m + jnp.log2(total)
            base[query, 1:2] = (mine[2, here] * ea + other[2, there] * eb) / total
            base[query, 2:8] = jnp.zeros((6, width), jnp.float32)
        dq[...] = jnp.zeros_like(dq)
    dk[...] = jnp.zeros_like(dk)
    dv[...] = jnp.zeros_like(dv)
    for block in range(len(blocks)):
        kt[block] = kv[2 * block].T
    factor = scale * LOG2E
    slots = [tiles[2 * i : 2 * i + 2] for i in range(4)]

    def entry(n):
        query, j0, b0, j1, b1 = entry_of(lists, n, key_blocks)
        return query, j0 - low, b0, j1 - low, b1

    def load(n, slot):
        score_tiles(entry(n), factor, qg, kv, bias, *slots[slot])

    def use(n, slot):
        query, j0, _, j1, _ = entry(n)
        t_ref, d_ref = slots[slot]
        p = jnp.exp2(t_ref[...] - base[query, 0:1])
        ds = (p * (d_ref[...] - base[query, 1:2])).astype(jnp.bfloat16)
        p = p.astype(jnp.bfloat16)
        dv_part = jnp.dot(p, qg[2 * query + 1], preferred_element_type=jnp.float32)
        dk_part = jnp.dot(ds, qg[2 * query], preferred_element_type=jnp.float32)
        kt2 = jnp.concatenate([kt[j0], kt[j1]], axis=1)
        dq[query] += jnp.dot(kt2, ds, preferred_element_type=jnp.float32)
        dk[j0] += dk_part[:size]
        dv[j0] += dv_part[:size]
        dk[j1] += dk_part[size:]
        dv[j1] += dv_part[size:]

    pair_loop(trips, load, use)
    for i in range(len(steps)):
        for half in range(2):
            for core in range(2):
                dst, row = (sent, 4 * i * size) if core else (outs[i], 0)
                row += 2 * half * size
                block = i * 4 + core * 2 + half
                dst[pl.ds(row, size), :] = (dk[block] * scale).astype(dst.dtype)
                dst[pl.ds(row + size, size), :] = dv[block].astype(dst.dtype)
    if last:
        for query in range(8):
            t, half = query // 2, query % 2
            dst, row = (sent, 4 * len(steps) * size) if t == 1 else (tops[max(t - 1, 0)], 0)
            for head in range(pairs):
                dst[pl.ds(row + (head * 2 + half) * size, size), :] = (
                    dq[query, :, pl.ds(head * size, size)].T * scale
                ).astype(dst.dtype)
    else:
        tops[0][...] = dq[...]
        tops[1][...] = base[...]


def attention_grads(queries, keys, values, out_grad, block_place):
    row_count, size = keys.shape
    block_len = row_count // 2
    pairs = queries.shape[1] // size // 2
    width = pairs * block_len
    outer_size = lax.axis_size("outer")
    key_blocks = STEPS * 4
    scale = 1.0 / math.sqrt(size)
    inner = lax.axis_index("inner")
    outer = lax.axis_index("outer")
    where = jnp.concatenate(
        [jnp.stack([inner, inner ^ 1, inner ^ 2, inner ^ 3, outer] + [outer] * 3), block_place]
    )
    smem = pl.BlockSpec(memory_space=pltpu.SMEM)
    vmem = pl.BlockSpec(memory_space=pltpu.VMEM)
    params = pltpu.CompilerParams(vmem_limit_bytes=16 << 20)
    low, full = jnp.bfloat16, jnp.float32

    q_shape, kv_shape = (4 * width, size), (4 * block_len, size)
    kv = jnp.stack(
        [keys.reshape(2, block_len, size), values.reshape(2, block_len, size)], axis=1
    ).reshape(kv_shape)
    own2 = from_behind(kv, "outer", 2)
    near_core = inner % 2

    def heads_of(array, core):
        split = array.reshape(2, block_len, 2, pairs, size)
        return lax.dynamic_index_in_dim(split, core, 2, False).transpose(0, 2, 1, 3)

    def packed(core):
        both = [heads_of(queries, core), heads_of(out_grad, core)]
        return jnp.stack(both, axis=1).reshape(q_shape)

    mine, theirs = packed(near_core), packed(1 - near_core)
    asked = [mine, swap(theirs, "inner", 1), swap(mine, "inner", 2), swap(theirs, "inner", 3)]
    own1 = swap(jnp.where(outer % 2 == 1, own2, kv), "outer", 1)
    own3 = from_behind(own2, "outer", 1)
    own = [kv, own1, own2, own3]
    near = [swap(block, "inner", 1) for block in own]
    q_parts = [part.reshape(4, width, size) for part in asked]
    shards = [block.reshape(4, block_len, size) for two in zip(own, near) for block in two]

    sizes = (outer_size, key_blocks, size, width)
    flops = 2 * 2 * width * 8 * key_blocks * block_len * size
    tile = pltpu.VMEM((2 * block_len, width), full)
    bias_table = pltpu.VMEM((3, block_len, block_len), full)

    def stats_call(steps, *early):
        merged = len(early) > 0
        count = 8 if merged else 4
        held = range(STEPS) if merged else steps
        used = [part for step in held for part in shards[2 * step : 2 * step + 2]]
        return pl.pallas_call(
            functools.partial(stats_kernel, sizes, scale * LOG2E, steps, merged),
            name="stats",
            out_shape=jax.ShapeDtypeStruct((3, 8, width), full),
            in_specs=[smem] + [vmem] * (len(early) + count // 2 + len(used)),
            out_specs=vmem,
            scratch_shapes=[
                pltpu.VMEM((2 * count, width, size), low),
                pltpu.VMEM((4 * len(used), block_len, size), low),
                bias_table,
                *[tile, tile, pltpu.VMEM((8, width), full)] * 4,
                pltpu.VMEM((3, count, 8, width), full),
                pltpu.SMEM((count * key_blocks + 16,), jnp.int32),
            ],
            compiler_params=params,
            cost_estimate=pl.CostEstimate(
                flops=flops * 3 // 4 if merged else flops // 4, bytes_accessed=1 << 20, transcendentals=0
            ),
        )(where, *early, *q_parts[: count // 2], *used)

    early = stats_call((0, 2))
    stats = stats_call((1, 3), early)
    others = swap(stats, "inner", 2)
    shard_f32 = jax.ShapeDtypeStruct(kv_shape, full)
    rows = kv_shape[0]

    def grads_call(steps, last, *extra):
        n = len(steps)
        if last:
            tops = [
                jax.ShapeDtypeStruct((pairs * row_count, size), kind) for kind in (full, low, low)
            ]
        else:
            tops = [
                jax.ShapeDtypeStruct((8, size, width), full),
                jax.ShapeDtypeStruct((8, 8, width), full),
            ]
        used = [part for step in steps for part in shards[2 * step : 2 * step + 2]]
        return pl.pallas_call(
            functools.partial(grads_kernel, sizes, scale, steps, last),
            name="grads",
            out_shape=[shard_f32] * n
            + [jax.ShapeDtypeStruct((n * rows + (pairs * row_count if last else 0), size), low)]
            + tops,
            in_specs=[smem] + [vmem] * (len(extra) + 4 + 2 * n),
            out_specs=[vmem] * (n + 1 + len(tops)),
            scratch_shapes=[
                pltpu.VMEM((16, width, size), low),
                pltpu.VMEM((8 * n, block_len, size), low),
                pltpu.VMEM((4 * n, size, block_len), low),
                pltpu.VMEM((4 * n, block_len, size), full),
                pltpu.VMEM((4 * n, block_len, size), full),
                pltpu.VMEM((8, size, width), full),
                pltpu.VMEM((8, 8, width), full),
                bias_table,
                *[tile] * 8,
                pltpu.SMEM((8 * 4 * n + 16,), jnp.int32),
            ],
            compiler_params=params,
            cost_estimate=pl.CostEstimate(
                flops=flops * 3 * n // STEPS, bytes_accessed=1 << 21, transcendentals=0
            ),
        )(where, *extra, *q_parts, *used)

    far_steps = tuple(range(STEPS // 2, STEPS))
    near_steps = tuple(range(STEPS // 2))
    *far_own, sent, dq_carry, base = grads_call(far_steps, False, stats, others)
    far_got = swap(sent, "inner", 1)
    *near_own, sent, dq0, dq2, dq3 = grads_call(near_steps, True, dq_carry, base)
    near_got = swap(sent, "inner", 1)
    back = []
    for steps, parts, got in ((far_steps, far_own, far_got), (near_steps, near_own, near_got)):
        for i, step in enumerate(steps):
            whole = parts[i] + got[i * rows : (i + 1) * rows].astype(full)
            if step > 0:
                whole = from_behind(whole.astype(low), "outer", -step)
            back.append(whole.astype(full))
    heads_mine = dq0 + swap(dq2, "inner", 2).astype(full)
    heads_other = near_got[len(near_steps) * rows :].astype(full) + swap(dq3, "inner", 3).astype(full)
    first = near_core == 0
    dq = jnp.concatenate(
        [
            part.reshape(pairs, row_count, size)[head]
            for part in (jnp.where(first, heads_mine, heads_other), jnp.where(first, heads_other, heads_mine))
            for head in range(pairs)
        ],
        axis=1,
    )
    back.reverse()
    total = sum(back[1:], back[0]).astype(low).reshape(2, 2, block_len, size)
    return (
        dq.astype(low),
        total[:, 0].reshape(row_count, size),
        total[:, 1].reshape(row_count, size),
    )


def solution(mesh):
    placed = (
        P(("inner", "outer"), None),
        P(("inner", "outer"), None),
        P(("inner", "outer"), None),
        P(("inner", "outer"), None),
        P(),
    )
    return jax.shard_map(
        attention_grads,
        mesh=mesh,
        in_specs=placed,
        out_specs=(
            P(("inner", "outer"), None),
            P(("inner", "outer"), None),
            P(("inner", "outer"), None),
        ),
        check_vma=False,
    )
```

```python
import functools
import math

import jax
import jax.numpy as jnp
from jax import lax
from jax.experimental import pallas as pl
from jax.experimental.pallas import tpu as pltpu
from jax.sharding import PartitionSpec as P


STEPS = 4
NEG = -1e30
LOG2E = math.log2(math.e)
NT = (((1,), (1,)), ((), ()))


def dot_nt(a, b):
    return lax.dot_general(a, b, NT, preferred_element_type=jnp.float32)


def from_behind(block, axis, distance):
    devices = range(lax.axis_size(axis))
    route = [((i - distance) % len(devices), i) for i in devices]
    return lax.ppermute(block, axis, route)


def swap(block, axis, bit):
    return lax.ppermute(block, axis, [(i, i ^ bit) for i in range(lax.axis_size(axis))])


def fill_bias(bias_ref):
    size = bias_ref.shape[1]
    key_off = lax.broadcasted_iota(jnp.int32, (size, size), 0)
    query_off = lax.broadcasted_iota(jnp.int32, (size, size), 1)
    bias_ref[0] = jnp.zeros((size, size), jnp.float32)
    bias_ref[1] = jnp.where(key_off <= query_off, 0.0, NEG).astype(jnp.float32)
    bias_ref[2] = jnp.full((size, size), NEG, jnp.float32)


def build_list(sizes, plan, where_ref, list_ref):
    outer_size, key_blocks = sizes
    outer = where_ref[4]
    key_place = {}
    for block in sorted({block for _, blocks in plan for block in blocks}):
        step, core, half = block // 4, (block // 2) % 2, block % 2
        source = lax.rem(outer - step + outer_size, outer_size)
        key_place[block] = where_ref[8 + (where_ref[core] * outer_size + source) * 2 + half]
    position = jnp.int32(0)
    pad = (plan[0][0] * key_blocks + plan[0][1][0]) * 4 + 2
    for query, blocks in plan:
        query_place = where_ref[8 + (where_ref[query // 2] * outer_size + outer) * 2 + query % 2]
        for block in blocks:
            kind = jnp.where(key_place[block] == query_place, 1, 0)
            list_ref[position] = (query * key_blocks + block) * 4 + kind
            position = position + jnp.where(key_place[block] <= query_place, 1, 0)
        list_ref[position] = (query * key_blocks + blocks[0]) * 4 + 2
        position = position + lax.rem(position, 2)
    for extra in range(10):
        list_ref[position + extra] = pad
    trips = (position + 6) // 8
    list_ref[list_ref.shape[0] - 1] = trips
    return trips


def list_size(plan):
    return sum(len(blocks) for _, blocks in plan) + 16


def stats_plan(steps, merged):
    held = range(STEPS) if merged else steps
    order = (list(range(4, 8)) if merged else []) + list(range(4))
    return [(query, blocks_of(held if query >= 4 else steps)) for query in order]


def grads_plan(steps):
    return [(query, blocks_of(steps)) for query in range(8)]


def blocks_of(steps):
    return [4 * step + i for step in steps for i in range(4)]


def entry_of(list_ref, index, key_blocks):
    e0, e1 = list_ref[2 * index], list_ref[2 * index + 1]
    at0, at1 = e0 // 4, e1 // 4
    return at0 // key_blocks, at0 % key_blocks, e0 % 4, at1 % key_blocks, e1 % 4


def score_tiles(entry, factor, qg, kv, bias):
    query, j0, b0, j1, b1 = entry
    k2 = jnp.concatenate([kv[2 * j0], kv[2 * j1]], axis=0)
    v2 = jnp.concatenate([kv[2 * j0 + 1], kv[2 * j1 + 1]], axis=0)
    low, high = bias[b0], bias[b1]
    b2 = jnp.concatenate(
        [jnp.concatenate([low, low], axis=1), jnp.concatenate([high, high], axis=1)], axis=0
    )
    t = dot_nt(k2, qg[2 * query]) * factor + b2
    return t, dot_nt(v2, qg[2 * query + 1])


def stack_refs(refs, dst):
    for i, src in enumerate(refs):
        count = src.shape[0]
        dst[pl.ds(i * count, count)] = src[...]


def pair_loop(trips, load, use):
    load(0, 0)
    load(1, 1)

    @pl.loop(0, trips)
    def _(i):
        load(4 * i + 2, 2)
        load(4 * i + 3, 3)
        use(4 * i, 0)
        use(4 * i + 1, 1)
        load(4 * i + 4, 0)
        load(4 * i + 5, 1)
        use(4 * i + 2, 2)
        use(4 * i + 3, 3)


def stats_kernel(sizes, factor, steps, merged, later, where_ref, *rest):
    outer_size, key_blocks, _, width = sizes
    if merged:
        early, rest = rest[0], rest[1:]
    count = 8 if merged else 4
    held = list(range(STEPS)) if merged else list(steps)
    q_refs, kv_refs = rest[: count // 2], rest[count // 2 : count // 2 + 2 * len(held)]
    rest = rest[count // 2 + 2 * len(held) :]
    out_ref, later_refs, rest = rest[0], rest[1 : 1 + len(later)], rest[1 + len(later) :]
    qg, kv, bias, *tiles, state, lists = rest
    stack_refs(kv_refs, kv)
    stack_refs(q_refs, qg)
    if merged:
        lists = where_ref
        trips = lists[lists.shape[0] - 1]
    else:
        trips = build_list((outer_size, key_blocks), stats_plan(steps, merged), where_ref, lists)
    for plan, list_ref in zip(later, later_refs):
        build_list((outer_size, key_blocks), plan, where_ref, list_ref)
    fill_bias(bias)
    state[0] = jnp.full((count, 8, width), NEG, jnp.float32)
    state[1] = jnp.zeros((count, 8, width), jnp.float32)
    state[2] = jnp.zeros((count, 8, width), jnp.float32)
    if merged:
        for i in range(4):
            at = pl.ds(i, 1)
            state[0, i] = jnp.broadcast_to(early[0, at], (8, width))
            state[1, i, 0:1] = early[1, at]
            state[2, i, 0:1] = early[2, at]
    gap = held[1] - held[0]
    slots = [tiles[3 * i : 3 * i + 3] for i in range(4)]

    def slot_of(block):
        return block if gap == 1 else (block // 4 // gap) * 4 + block % 4

    def entry(n):
        query, j0, b0, j1, b1 = entry_of(lists, n, key_blocks)
        return query, slot_of(j0), b0, slot_of(j1), b1

    def load(n, slot):
        t_ref, d_ref, top = slots[slot]
        t, dp = score_tiles(entry(n), factor, qg, kv, bias)
        t_ref[...] = t
        top[...] = jnp.max(t.reshape(-1, 8, width), axis=0)
        d_ref[...] = dp

    def use(n, slot):
        query = entry(n)[0]
        t_ref, d_ref, top = slots[slot]
        m, l, r = state[0, query], state[1, query], state[2, query]
        m_new = jnp.maximum(m, jnp.max(top[...], axis=0, keepdims=True))
        corr = jnp.exp2(m - m_new)
        p = jnp.exp2(t_ref[...].reshape(-1, 8, width) - m_new)
        state[0, query] = m_new
        state[1, query] = l * corr + jnp.sum(p, axis=0)
        state[2, query] = r * corr + jnp.sum(p * d_ref[...].reshape(-1, 8, width), axis=0)

    pair_loop(trips, load, use)
    for i in range(count):
        at = pl.ds(i, 1)
        out_ref[0, at] = state[0, i, 0:1]
        out_ref[1, at] = jnp.sum(state[1, i], axis=0, keepdims=True)
        out_ref[2, at] = jnp.sum(state[2, i], axis=0, keepdims=True)
    if not merged:
        out_ref[:, pl.ds(count, count)] = jnp.zeros((3, count, width), jnp.float32)


def grads_kernel(sizes, scale, steps, last, lists, *rest):
    _, key_blocks, size, width = sizes
    pairs = width // size
    carry_in, rest = rest[:2], rest[2:]
    q_refs, kv_refs = rest[:4], rest[4 : 4 + 2 * len(steps)]
    rest = rest[4 + 2 * len(steps) :]
    outs, sent, rest = rest[: len(steps)], rest[len(steps)], rest[len(steps) + 1 :]
    tops, rest = rest[: (3 if last else 2)], rest[(3 if last else 2) :]
    qg, kv, kt, dk, dv, dq, base, bias, *tiles = rest
    low = 4 * min(steps)
    blocks = blocks_of(steps)
    stack_refs(kv_refs, kv)
    stack_refs(q_refs, qg)
    if last:
        dq[...] = carry_in[0][...]
        base[...] = carry_in[1][...]
    trips = lists[lists.shape[0] - 1]
    fill_bias(bias)
    if not last:
        for query in range(8):
            here, there = pl.ds(query, 1), pl.ds(query ^ 4, 1)
            mine, other = carry_in
            m = jnp.maximum(mine[0, here], other[0, there])
            ea, eb = jnp.exp2(mine[0, here] - m), jnp.exp2(other[0, there] - m)
            total = mine[1, here] * ea + other[1, there] * eb
            base[query, 0:1] = m + jnp.log2(total)
            base[query, 1:2] = (mine[2, here] * ea + other[2, there] * eb) / total
            base[query, 2:8] = jnp.zeros((6, width), jnp.float32)
        dq[...] = jnp.zeros_like(dq)
    dk[...] = jnp.zeros_like(dk)
    dv[...] = jnp.zeros_like(dv)
    for block in range(len(blocks)):
        kt[block] = kv[2 * block].T
    factor = scale * LOG2E
    slots = [tiles[2 * i : 2 * i + 2] for i in range(4)]

    def entry(n):
        query, j0, b0, j1, b1 = entry_of(lists, n, key_blocks)
        return query, j0 - low, b0, j1 - low, b1

    def load(n, slot):
        at = entry(n)
        p_ref, s_ref = slots[slot]
        t, dp = score_tiles(at, factor, qg, kv, bias)
        p = jnp.exp2(t - base[at[0], 0:1])
        p_ref[...] = p.astype(jnp.bfloat16)
        s_ref[...] = (p * (dp - base[at[0], 1:2])).astype(jnp.bfloat16)

    def use(n, slot):
        query, j0, _, j1, _ = entry(n)
        p, ds = slots[slot][0][...], slots[slot][1][...]
        dv_part = jnp.dot(p, qg[2 * query + 1], preferred_element_type=jnp.float32)
        dk_part = jnp.dot(ds, qg[2 * query], preferred_element_type=jnp.float32)
        kt2 = jnp.concatenate([kt[j0], kt[j1]], axis=1)
        dq[query] += jnp.dot(kt2, ds, preferred_element_type=jnp.float32)
        dk[j0] += dk_part[:size]
        dv[j0] += dv_part[:size]
        dk[j1] += dk_part[size:]
        dv[j1] += dv_part[size:]

    pair_loop(trips, load, use)
    for i in range(len(steps)):
        for half in range(2):
            for core in range(2):
                dst, row = (sent, 4 * i * size) if core else (outs[i], 0)
                row += 2 * half * size
                block = i * 4 + core * 2 + half
                dst[pl.ds(row, size), :] = (dk[block] * scale).astype(dst.dtype)
                dst[pl.ds(row + size, size), :] = dv[block].astype(dst.dtype)
    if last:
        for query in range(8):
            t, half = query // 2, query % 2
            dst, row = (sent, 4 * len(steps) * size) if t == 1 else (tops[max(t - 1, 0)], 0)
            for head in range(pairs):
                dst[pl.ds(row + (head * 2 + half) * size, size), :] = (
                    dq[query, :, pl.ds(head * size, size)].T * scale
                ).astype(dst.dtype)
    else:
        tops[0][...] = dq[...]
        tops[1][...] = base[...]


def attention_grads(queries, keys, values, out_grad, block_place):
    row_count, size = keys.shape
    block_len = row_count // 2
    pairs = queries.shape[1] // size // 2
    width = pairs * block_len
    outer_size = lax.axis_size("outer")
    key_blocks = STEPS * 4
    scale = 1.0 / math.sqrt(size)
    inner = lax.axis_index("inner")
    outer = lax.axis_index("outer")
    where = jnp.concatenate(
        [jnp.stack([inner, inner ^ 1, inner ^ 2, inner ^ 3, outer] + [outer] * 3), block_place]
    )
    smem = pl.BlockSpec(memory_space=pltpu.SMEM)
    vmem = pl.BlockSpec(memory_space=pltpu.VMEM)
    params = pltpu.CompilerParams(vmem_limit_bytes=16 << 20)
    low, full = jnp.bfloat16, jnp.float32

    q_shape, kv_shape = (4 * width, size), (4 * block_len, size)
    kv = jnp.stack(
        [keys.reshape(2, block_len, size), values.reshape(2, block_len, size)], axis=1
    ).reshape(kv_shape)
    own2 = from_behind(kv, "outer", 2)
    near_core = inner % 2

    def heads_of(array, core):
        split = array.reshape(2, block_len, 2, pairs, size)
        return lax.dynamic_index_in_dim(split, core, 2, False).transpose(0, 2, 1, 3)

    def packed(core):
        both = [heads_of(queries, core), heads_of(out_grad, core)]
        return jnp.stack(both, axis=1).reshape(q_shape)

    mine, theirs = packed(near_core), packed(1 - near_core)
    asked = [mine, swap(theirs, "inner", 1), swap(mine, "inner", 2), swap(theirs, "inner", 3)]
    own1 = swap(jnp.where(outer % 2 == 1, own2, kv), "outer", 1)
    own3 = from_behind(own2, "outer", 1)
    own = [kv, own1, own2, own3]
    near = [swap(block, "inner", 1) for block in own]
    q_parts = [part.reshape(4, width, size) for part in asked]
    shards = [block.reshape(4, block_len, size) for two in zip(own, near) for block in two]

    sizes = (outer_size, key_blocks, size, width)
    far_steps = tuple(range(STEPS // 2, STEPS))
    near_steps = tuple(range(STEPS // 2))
    flops = 2 * 2 * width * 8 * key_blocks * block_len * size
    tile = pltpu.VMEM((2 * block_len, width), full)
    bias_table = pltpu.VMEM((3, block_len, block_len), full)

    def stats_call(table, steps, later, *early):
        merged = len(early) > 0
        count = 8 if merged else 4
        held = range(STEPS) if merged else steps
        used = [part for step in held for part in shards[2 * step : 2 * step + 2]]
        return pl.pallas_call(
            functools.partial(stats_kernel, sizes, scale * LOG2E, steps, merged, later),
            name="stats",
            out_shape=[jax.ShapeDtypeStruct((3, 8, width), full)]
            + [jax.ShapeDtypeStruct((list_size(plan),), jnp.int32) for plan in later],
            in_specs=[smem] + [vmem] * (len(early) + count // 2 + len(used)),
            out_specs=[vmem] + [smem] * len(later),
            scratch_shapes=[
                pltpu.VMEM((2 * count, width, size), low),
                pltpu.VMEM((4 * len(used), block_len, size), low),
                bias_table,
                *[tile, tile, pltpu.VMEM((8, width), full)] * 4,
                pltpu.VMEM((3, count, 8, width), full),
                pltpu.SMEM((count * key_blocks + 16,), jnp.int32),
            ],
            compiler_params=params,
            cost_estimate=pl.CostEstimate(
                flops=flops * 3 // 4 if merged else flops // 4, bytes_accessed=1 << 20, transcendentals=0
            ),
        )(table, *early, *q_parts[: count // 2], *used)

    early, rest_list, far_list, near_list = stats_call(
        where, (0, 2), (stats_plan((1, 3), True), grads_plan(far_steps), grads_plan(near_steps))
    )
    (stats,) = stats_call(rest_list, (1, 3), (), early)
    others = swap(stats, "inner", 2)
    shard_f32 = jax.ShapeDtypeStruct(kv_shape, full)
    rows = kv_shape[0]

    def grads_call(table, steps, last, *extra):
        n = len(steps)
        if last:
            tops = [
                jax.ShapeDtypeStruct((pairs * row_count, size), kind) for kind in (full, low, low)
            ]
        else:
            tops = [
                jax.ShapeDtypeStruct((8, size, width), full),
                jax.ShapeDtypeStruct((8, 8, width), full),
            ]
        used = [part for step in steps for part in shards[2 * step : 2 * step + 2]]
        return pl.pallas_call(
            functools.partial(grads_kernel, sizes, scale, steps, last),
            name="grads",
            out_shape=[shard_f32] * n
            + [jax.ShapeDtypeStruct((n * rows + (pairs * row_count if last else 0), size), low)]
            + tops,
            in_specs=[smem] + [vmem] * (len(extra) + 4 + 2 * n),
            out_specs=[vmem] * (n + 1 + len(tops)),
            scratch_shapes=[
                pltpu.VMEM((16, width, size), low),
                pltpu.VMEM((8 * n, block_len, size), low),
                pltpu.VMEM((4 * n, size, block_len), low),
                pltpu.VMEM((4 * n, block_len, size), full),
                pltpu.VMEM((4 * n, block_len, size), full),
                pltpu.VMEM((8, size, width), full),
                pltpu.VMEM((8, 8, width), full),
                bias_table,
                *[pltpu.VMEM((2 * block_len, width), low)] * 8,
            ],
            compiler_params=params,
            cost_estimate=pl.CostEstimate(
                flops=flops * 3 * n // STEPS, bytes_accessed=1 << 21, transcendentals=0
            ),
        )(table, *extra, *q_parts, *used)

    *far_own, sent, dq_carry, base = grads_call(far_list, far_steps, False, stats, others)
    far_got = swap(sent, "inner", 1)
    *near_own, sent, dq0, dq2, dq3 = grads_call(near_list, near_steps, True, dq_carry, base)
    near_got = swap(sent, "inner", 1)
    back = []
    for steps, parts, got in ((far_steps, far_own, far_got), (near_steps, near_own, near_got)):
        for i, step in enumerate(steps):
            whole = parts[i] + got[i * rows : (i + 1) * rows].astype(full)
            if step > 0:
                whole = from_behind(whole.astype(low), "outer", -step)
            back.append(whole.astype(full))
    heads_mine = dq0 + swap(dq2, "inner", 2).astype(full)
    heads_other = near_got[len(near_steps) * rows :].astype(full) + swap(dq3, "inner", 3).astype(full)
    first = near_core == 0
    dq = jnp.concatenate(
        [
            part.reshape(pairs, row_count, size)[head]
            for part in (jnp.where(first, heads_mine, heads_other), jnp.where(first, heads_other, heads_mine))
            for head in range(pairs)
        ],
        axis=1,
    )
    back.reverse()
    total = sum(back[1:], back[0]).astype(low).reshape(2, 2, block_len, size)
    return (
        dq.astype(low),
        total[:, 0].reshape(row_count, size),
        total[:, 1].reshape(row_count, size),
    )


def solution(mesh):
    placed = (
        P(("inner", "outer"), None),
        P(("inner", "outer"), None),
        P(("inner", "outer"), None),
        P(("inner", "outer"), None),
        P(),
    )
    return jax.shard_map(
        attention_grads,
        mesh=mesh,
        in_specs=placed,
        out_specs=(
            P(("inner", "outer"), None),
            P(("inner", "outer"), None),
            P(("inner", "outer"), None),
        ),
        check_vma=False,
    )
```

```python
import functools
import math

import jax
import jax.numpy as jnp
from jax import lax
from jax.experimental import pallas as pl
from jax.experimental.pallas import tpu as pltpu
from jax.sharding import PartitionSpec as P


STEPS = 4
NEG = -1e30
LOG2E = math.log2(math.e)
NT = (((1,), (1,)), ((), ()))


def dot_nt(a, b):
    return lax.dot_general(a, b, NT, preferred_element_type=jnp.float32)


def from_behind(block, axis, distance):
    devices = range(lax.axis_size(axis))
    route = [((i - distance) % len(devices), i) for i in devices]
    return lax.ppermute(block, axis, route)


def swap(block, axis, bit):
    return lax.ppermute(block, axis, [(i, i ^ bit) for i in range(lax.axis_size(axis))])


def fill_bias(bias_ref):
    size = bias_ref.shape[1]
    key_off = lax.broadcasted_iota(jnp.int32, (size, size), 0)
    query_off = lax.broadcasted_iota(jnp.int32, (size, size), 1)
    bias_ref[0] = jnp.zeros((size, size), jnp.float32)
    bias_ref[1] = jnp.where(key_off <= query_off, 0.0, NEG).astype(jnp.float32)
    bias_ref[2] = jnp.full((size, size), NEG, jnp.float32)


def build_list(sizes, plan, where_ref, list_ref):
    outer_size, key_blocks = sizes
    outer = where_ref[4]
    key_place = {}
    for block in sorted({block for _, blocks in plan for block in blocks}):
        step, core, half = block // 4, (block // 2) % 2, block % 2
        source = lax.rem(outer - step + outer_size, outer_size)
        key_place[block] = where_ref[8 + (where_ref[core] * outer_size + source) * 2 + half]
    position = jnp.int32(0)
    pad = (plan[0][0] * key_blocks + plan[0][1][0]) * 4 + 2
    for query, blocks in plan:
        query_place = where_ref[8 + (where_ref[query // 2] * outer_size + outer) * 2 + query % 2]
        for block in blocks:
            kind = jnp.where(key_place[block] == query_place, 1, 0)
            list_ref[position] = (query * key_blocks + block) * 4 + kind
            position = position + jnp.where(key_place[block] <= query_place, 1, 0)
        list_ref[position] = (query * key_blocks + blocks[0]) * 4 + 2
        position = position + lax.rem(position, 2)
    for extra in range(10):
        list_ref[position + extra] = pad
    trips = (position + 6) // 8
    list_ref[list_ref.shape[0] - 1] = trips
    return trips


def list_size(plan):
    return sum(len(blocks) for _, blocks in plan) + 16


def stats_plan(steps, merged):
    held = range(STEPS) if merged else steps
    order = (list(range(4, 8)) if merged else []) + list(range(4))
    return [(query, blocks_of(held if query >= 4 else steps)) for query in order]


def grads_plan(steps):
    return [(query, blocks_of(steps)) for query in range(8)]


def blocks_of(steps):
    return [4 * step + i for step in steps for i in range(4)]


def entry_of(list_ref, index, key_blocks):
    e0, e1 = list_ref[2 * index], list_ref[2 * index + 1]
    at0, at1 = e0 // 4, e1 // 4
    return at0 // key_blocks, at0 % key_blocks, e0 % 4, at1 % key_blocks, e1 % 4


def score_tiles(entry, factor, qg, kv, bias):
    query, j0, b0, j1, b1 = entry
    k2 = jnp.concatenate([kv[2 * j0], kv[2 * j1]], axis=0)
    v2 = jnp.concatenate([kv[2 * j0 + 1], kv[2 * j1 + 1]], axis=0)
    low, high = bias[b0], bias[b1]
    b2 = jnp.concatenate(
        [jnp.concatenate([low, low], axis=1), jnp.concatenate([high, high], axis=1)], axis=0
    )
    t = dot_nt(k2, qg[2 * query]) * factor + b2
    return t, dot_nt(v2, qg[2 * query + 1])


def stack_refs(refs, dst):
    for i, src in enumerate(refs):
        count = src.shape[0]
        dst[pl.ds(i * count, count)] = src[...]


def pair_loop(trips, load, use):
    load(0, 0)
    load(1, 1)

    @pl.loop(0, trips)
    def _(i):
        load(4 * i + 2, 2)
        load(4 * i + 3, 3)
        use(4 * i, 0)
        use(4 * i + 1, 1)
        load(4 * i + 4, 0)
        load(4 * i + 5, 1)
        use(4 * i + 2, 2)
        use(4 * i + 3, 3)


def stats_kernel(sizes, factor, steps, merged, later, where_ref, *rest):
    outer_size, key_blocks, _, width = sizes
    if merged:
        early, rest = rest[0], rest[1:]
    count = 8 if merged else 4
    held = list(range(STEPS)) if merged else list(steps)
    q_refs, kv_refs = rest[: count // 2], rest[count // 2 : count // 2 + 2 * len(held)]
    rest = rest[count // 2 + 2 * len(held) :]
    out_ref, later_refs, rest = rest[0], rest[1 : 1 + len(later)], rest[1 + len(later) :]
    qg, kv, bias, *tiles, state, lists = rest
    stack_refs(kv_refs, kv)
    stack_refs(q_refs, qg)
    if merged:
        lists = where_ref
        trips = lists[lists.shape[0] - 1]
    else:
        trips = build_list((outer_size, key_blocks), stats_plan(steps, merged), where_ref, lists)
    for plan, list_ref in zip(later, later_refs):
        build_list((outer_size, key_blocks), plan, where_ref, list_ref)
    fill_bias(bias)
    state[0] = jnp.full((count, 8, width), NEG, jnp.float32)
    state[1] = jnp.zeros((count, 8, width), jnp.float32)
    state[2] = jnp.zeros((count, 8, width), jnp.float32)
    if merged:
        for i in range(4):
            at = pl.ds(i, 1)
            state[0, i] = jnp.broadcast_to(early[0, at], (8, width))
            state[1, i, 0:1] = early[1, at]
            state[2, i, 0:1] = early[2, at]
    gap = held[1] - held[0]
    slots = [tiles[3 * i : 3 * i + 3] for i in range(4)]

    def slot_of(block):
        return block if gap == 1 else (block // 4 // gap) * 4 + block % 4

    def entry(n):
        query, j0, b0, j1, b1 = entry_of(lists, n, key_blocks)
        return query, slot_of(j0), b0, slot_of(j1), b1

    def load(n, slot):
        t_ref, d_ref, top = slots[slot]
        t, dp = score_tiles(entry(n), factor, qg, kv, bias)
        t_ref[...] = t
        top[...] = jnp.max(t.reshape(-1, 8, width), axis=0)
        d_ref[...] = dp.astype(jnp.bfloat16)

    def use(n, slot):
        query = entry(n)[0]
        t_ref, d_ref, top = slots[slot]
        m, l, r = state[0, query], state[1, query], state[2, query]
        m_new = jnp.maximum(m, jnp.max(top[...], axis=0, keepdims=True))
        corr = jnp.exp2(m - m_new)
        p = jnp.exp2(t_ref[...].reshape(-1, 8, width) - m_new)
        state[0, query] = m_new
        state[1, query] = l * corr + jnp.sum(p, axis=0)
        state[2, query] = r * corr + jnp.sum(p * d_ref[...].astype(jnp.float32).reshape(-1, 8, width), axis=0)

    pair_loop(trips, load, use)
    for i in range(count):
        at = pl.ds(i, 1)
        out_ref[0, at] = state[0, i, 0:1]
        out_ref[1, at] = jnp.sum(state[1, i], axis=0, keepdims=True)
        out_ref[2, at] = jnp.sum(state[2, i], axis=0, keepdims=True)
    if not merged:
        out_ref[:, pl.ds(count, count)] = jnp.zeros((3, count, width), jnp.float32)


def grads_kernel(sizes, scale, steps, last, lists, *rest):
    _, key_blocks, size, width = sizes
    pairs = width // size
    carry_in, rest = rest[:2], rest[2:]
    q_refs, kv_refs = rest[:4], rest[4 : 4 + 2 * len(steps)]
    rest = rest[4 + 2 * len(steps) :]
    outs, sent, rest = rest[: len(steps)], rest[len(steps)], rest[len(steps) + 1 :]
    tops, rest = rest[: (3 if last else 2)], rest[(3 if last else 2) :]
    qg, kv, kt, dk, dv, dq, base, bias, *tiles = rest
    low = 4 * min(steps)
    blocks = blocks_of(steps)
    stack_refs(kv_refs, kv)
    stack_refs(q_refs, qg)
    if last:
        dq[...] = carry_in[0][...]
        base[...] = carry_in[1][...]
    trips = lists[lists.shape[0] - 1]
    fill_bias(bias)
    if not last:
        for query in range(8):
            here, there = pl.ds(query, 1), pl.ds(query ^ 4, 1)
            mine, other = carry_in
            m = jnp.maximum(mine[0, here], other[0, there])
            ea, eb = jnp.exp2(mine[0, here] - m), jnp.exp2(other[0, there] - m)
            total = mine[1, here] * ea + other[1, there] * eb
            base[query, 0:1] = m + jnp.log2(total)
            base[query, 1:2] = (mine[2, here] * ea + other[2, there] * eb) / total
            base[query, 2:8] = jnp.zeros((6, width), jnp.float32)
        dq[...] = jnp.zeros_like(dq)
    dk[...] = jnp.zeros_like(dk)
    dv[...] = jnp.zeros_like(dv)
    for block in range(len(blocks)):
        kt[block] = kv[2 * block].T
    factor = scale * LOG2E
    slots = [tiles[2 * i : 2 * i + 2] for i in range(4)]

    def entry(n):
        query, j0, b0, j1, b1 = entry_of(lists, n, key_blocks)
        return query, j0 - low, b0, j1 - low, b1

    def load(n, slot):
        at = entry(n)
        p_ref, s_ref = slots[slot]
        t, dp = score_tiles(at, factor, qg, kv, bias)
        p = jnp.exp2(t - base[at[0], 0:1])
        p_ref[...] = p.astype(jnp.bfloat16)
        s_ref[...] = (p * (dp - base[at[0], 1:2])).astype(jnp.bfloat16)

    def use(n, slot):
        query, j0, _, j1, _ = entry(n)
        p, ds = slots[slot][0][...], slots[slot][1][...]
        dv_part = jnp.dot(p, qg[2 * query + 1], preferred_element_type=jnp.float32)
        dk_part = jnp.dot(ds, qg[2 * query], preferred_element_type=jnp.float32)
        kt2 = jnp.concatenate([kt[j0], kt[j1]], axis=1)
        dq[query] += jnp.dot(kt2, ds, preferred_element_type=jnp.float32)
        dk[j0] += dk_part[:size]
        dv[j0] += dv_part[:size]
        dk[j1] += dk_part[size:]
        dv[j1] += dv_part[size:]

    pair_loop(trips, load, use)
    for i in range(len(steps)):
        for half in range(2):
            for core in range(2):
                dst, row = (sent, 4 * i * size) if core else (outs[i], 0)
                row += 2 * half * size
                block = i * 4 + core * 2 + half
                dst[pl.ds(row, size), :] = (dk[block] * scale).astype(dst.dtype)
                dst[pl.ds(row + size, size), :] = dv[block].astype(dst.dtype)
    if last:
        for query in range(8):
            t, half = query // 2, query % 2
            dst, row = (sent, 4 * len(steps) * size) if t == 1 else (tops[max(t - 1, 0)], 0)
            for head in range(pairs):
                dst[pl.ds(row + (head * 2 + half) * size, size), :] = (
                    dq[query, :, pl.ds(head * size, size)].T * scale
                ).astype(dst.dtype)
    else:
        tops[0][...] = dq[...]
        tops[1][...] = base[...]


def attention_grads(queries, keys, values, out_grad, block_place):
    row_count, size = keys.shape
    block_len = row_count // 2
    pairs = queries.shape[1] // size // 2
    width = pairs * block_len
    outer_size = lax.axis_size("outer")
    key_blocks = STEPS * 4
    scale = 1.0 / math.sqrt(size)
    inner = lax.axis_index("inner")
    outer = lax.axis_index("outer")
    where = jnp.concatenate(
        [jnp.stack([inner, inner ^ 1, inner ^ 2, inner ^ 3, outer] + [outer] * 3), block_place]
    )
    smem = pl.BlockSpec(memory_space=pltpu.SMEM)
    vmem = pl.BlockSpec(memory_space=pltpu.VMEM)
    params = pltpu.CompilerParams(vmem_limit_bytes=16 << 20)
    low, full = jnp.bfloat16, jnp.float32

    q_shape, kv_shape = (4 * width, size), (4 * block_len, size)
    kv = jnp.stack(
        [keys.reshape(2, block_len, size), values.reshape(2, block_len, size)], axis=1
    ).reshape(kv_shape)
    own2 = from_behind(kv, "outer", 2)
    near_core = inner % 2

    def heads_of(array, core):
        split = array.reshape(2, block_len, 2, pairs, size)
        return lax.dynamic_index_in_dim(split, core, 2, False).transpose(0, 2, 1, 3)

    def packed(core):
        both = [heads_of(queries, core), heads_of(out_grad, core)]
        return jnp.stack(both, axis=1).reshape(q_shape)

    mine, theirs = packed(near_core), packed(1 - near_core)
    asked = [mine, swap(theirs, "inner", 1), swap(mine, "inner", 2), swap(theirs, "inner", 3)]
    own1 = swap(jnp.where(outer % 2 == 1, own2, kv), "outer", 1)
    own3 = from_behind(own2, "outer", 1)
    own = [kv, own1, own2, own3]
    near = [swap(block, "inner", 1) for block in own]
    q_parts = [part.reshape(4, width, size) for part in asked]
    shards = [block.reshape(4, block_len, size) for two in zip(own, near) for block in two]

    sizes = (outer_size, key_blocks, size, width)
    far_steps = tuple(range(STEPS // 2, STEPS))
    near_steps = tuple(range(STEPS // 2))
    flops = 2 * 2 * width * 8 * key_blocks * block_len * size
    tile = pltpu.VMEM((2 * block_len, width), full)
    bias_table = pltpu.VMEM((3, block_len, block_len), full)

    def stats_call(table, steps, later, *early):
        merged = len(early) > 0
        count = 8 if merged else 4
        held = range(STEPS) if merged else steps
        used = [part for step in held for part in shards[2 * step : 2 * step + 2]]
        return pl.pallas_call(
            functools.partial(stats_kernel, sizes, scale * LOG2E, steps, merged, later),
            name="stats",
            out_shape=[jax.ShapeDtypeStruct((3, 8, width), full)]
            + [jax.ShapeDtypeStruct((list_size(plan),), jnp.int32) for plan in later],
            in_specs=[smem] + [vmem] * (len(early) + count // 2 + len(used)),
            out_specs=[vmem] + [smem] * len(later),
            scratch_shapes=[
                pltpu.VMEM((2 * count, width, size), low),
                pltpu.VMEM((4 * len(used), block_len, size), low),
                bias_table,
                *[tile, pltpu.VMEM((2 * block_len, width), low), pltpu.VMEM((8, width), full)] * 4,
                pltpu.VMEM((3, count, 8, width), full),
                pltpu.SMEM((count * key_blocks + 16,), jnp.int32),
            ],
            compiler_params=params,
            cost_estimate=pl.CostEstimate(
                flops=flops * 3 // 4 if merged else flops // 4, bytes_accessed=1 << 20, transcendentals=0
            ),
        )(table, *early, *q_parts[: count // 2], *used)

    early, rest_list, far_list, near_list = stats_call(
        where, (0, 2), (stats_plan((1, 3), True), grads_plan(far_steps), grads_plan(near_steps))
    )
    (stats,) = stats_call(rest_list, (1, 3), (), early)
    others = swap(stats, "inner", 2)
    shard_f32 = jax.ShapeDtypeStruct(kv_shape, full)
    rows = kv_shape[0]

    def grads_call(table, steps, last, *extra):
        n = len(steps)
        if last:
            tops = [
                jax.ShapeDtypeStruct((pairs * row_count, size), kind) for kind in (full, low, low)
            ]
        else:
            tops = [
                jax.ShapeDtypeStruct((8, size, width), full),
                jax.ShapeDtypeStruct((8, 8, width), full),
            ]
        used = [part for step in steps for part in shards[2 * step : 2 * step + 2]]
        return pl.pallas_call(
            functools.partial(grads_kernel, sizes, scale, steps, last),
            name="grads",
            out_shape=[shard_f32] * n
            + [jax.ShapeDtypeStruct((n * rows + (pairs * row_count if last else 0), size), low)]
            + tops,
            in_specs=[smem] + [vmem] * (len(extra) + 4 + 2 * n),
            out_specs=[vmem] * (n + 1 + len(tops)),
            scratch_shapes=[
                pltpu.VMEM((16, width, size), low),
                pltpu.VMEM((8 * n, block_len, size), low),
                pltpu.VMEM((4 * n, size, block_len), low),
                pltpu.VMEM((4 * n, block_len, size), full),
                pltpu.VMEM((4 * n, block_len, size), full),
                pltpu.VMEM((8, size, width), full),
                pltpu.VMEM((8, 8, width), full),
                bias_table,
                *[pltpu.VMEM((2 * block_len, width), low)] * 8,
            ],
            compiler_params=params,
            cost_estimate=pl.CostEstimate(
                flops=flops * 3 * n // STEPS, bytes_accessed=1 << 21, transcendentals=0
            ),
        )(table, *extra, *q_parts, *used)

    *far_own, sent, dq_carry, base = grads_call(far_list, far_steps, False, stats, others)
    far_got = swap(sent, "inner", 1)
    *near_own, sent, dq0, dq2, dq3 = grads_call(near_list, near_steps, True, dq_carry, base)
    near_got = swap(sent, "inner", 1)
    back = []
    for steps, parts, got in ((far_steps, far_own, far_got), (near_steps, near_own, near_got)):
        for i, step in enumerate(steps):
            whole = parts[i] + got[i * rows : (i + 1) * rows].astype(full)
            if step > 0:
                whole = from_behind(whole.astype(low), "outer", -step)
            back.append(whole.astype(full))
    heads_mine = dq0 + swap(dq2, "inner", 2).astype(full)
    heads_other = near_got[len(near_steps) * rows :].astype(full) + swap(dq3, "inner", 3).astype(full)
    first = near_core == 0
    dq = jnp.concatenate(
        [
            part.reshape(pairs, row_count, size)[head]
            for part in (jnp.where(first, heads_mine, heads_other), jnp.where(first, heads_other, heads_mine))
            for head in range(pairs)
        ],
        axis=1,
    )
    back.reverse()
    total = sum(back[1:], back[0]).astype(low).reshape(2, 2, block_len, size)
    return (
        dq.astype(low),
        total[:, 0].reshape(row_count, size),
        total[:, 1].reshape(row_count, size),
    )


def solution(mesh):
    placed = (
        P(("inner", "outer"), None),
        P(("inner", "outer"), None),
        P(("inner", "outer"), None),
        P(("inner", "outer"), None),
        P(),
    )
    return jax.shard_map(
        attention_grads,
        mesh=mesh,
        in_specs=placed,
        out_specs=(
            P(("inner", "outer"), None),
            P(("inner", "outer"), None),
            P(("inner", "outer"), None),
        ),
        check_vma=False,
    )
```
